32 devices in a mesh: dp: 2 (over x), sp: 16 (over y, z, core).
Axes of the slice: x: 2, y: 2, z: 4, core: 2. Of those that a mesh axis runs over, the one named last changes fastest.
Arguments:
- x: bfloat16 [16384, 2304], P(('dp', 'sp')), parts along dimension 0
- gain: bfloat16 [2304], replicated
- wq: bfloat16 [2304, 2048], P('sp')
- wk: bfloat16 [2304, 1024], P('sp')
- wv: bfloat16 [2304, 1024], P('sp')
- wo: bfloat16 [2048, 2304], P('sp')
Outputs:
- output: bfloat16 [16384, 2304], P(('dp', 'sp')), parts along dimension 0
There are 2 independent parts. The reference program is written for one: setup_inputs(seed, part) draws one part's arguments, and reference() takes and returns one part's arrays. A program takes and returns all parts, laid end to end along the dimension named above; an argument that names none is the same for every part.
All inputs are finite; a program needn't handle non-finite values.
Results may differ from the reference program's by a relative error of at most 0.012.
Values are sent between devices in bfloat16 or wider.
A program may use at most 2 GiB of HBM per device.

```python
import jax
import jax.numpy as jnp
from jax import lax

ROWS = 8192
D = 2304
HEADS = 8
KV_HEADS = 4
HEAD = 256
THETA = 10000


def setup_inputs(seed: int = 0, part: int = 0) -> dict:
    kx, kn, kq, kk, kv, ko = jax.random.split(jax.random.key(seed), 6)

    def weights(key, rows, columns):
        return jax.random.normal(key, (rows, columns), jnp.float32) * rows**-0.5

    drawn = {
        "x": jax.random.normal(jax.random.fold_in(kx, part), (ROWS, D), jnp.float32),
        "gain": 1 + 0.1 * jax.random.normal(kn, (D,), jnp.float32),
        "wq": 2 * weights(kq, D, HEADS * HEAD),
        "wk": 2 * weights(kk, D, KV_HEADS * HEAD),
        "wv": 4 * weights(kv, D, KV_HEADS * HEAD),
        "wo": weights(ko, HEADS * HEAD, D),
    }
    return {k: v.astype(jnp.bfloat16) for k, v in drawn.items()}


def normed(x, gain):
    wide = x.astype(jnp.float32)
    scale = lax.rsqrt(jnp.mean(wide * wide, -1, keepdims=True) + 1e-6)
    return (wide * scale * gain.astype(jnp.float32)).astype(jnp.bfloat16)


def turned(t, place, theta):
    half = t.shape[-1] // 2
    angle = place.astype(jnp.float32)[:, None] * theta ** (-jnp.arange(half, dtype=jnp.float32) / half)
    cos, sin = jnp.cos(angle)[:, None], jnp.sin(angle)[:, None]
    a, b = t[..., :half].astype(jnp.float32), t[..., half:].astype(jnp.float32)
    return jnp.concatenate([a * cos - b * sin, b * cos + a * sin], -1).astype(jnp.bfloat16)


def matmul(a, w):
    return jnp.dot(a, w, preferred_element_type=jnp.float32).astype(jnp.bfloat16)


def einsum(form, a, b):
    return jnp.einsum(form, a.astype(jnp.float32), b.astype(jnp.float32))


def attention(q, k, v):
    scores = einsum("tgsd,ugd->gstu", q, k) * q.shape[-1] ** -0.5
    token = jnp.arange(q.shape[0])
    scores = jnp.where(token[:, None] >= token, scores, -jnp.inf)
    weights = jax.nn.softmax(scores, -1).astype(jnp.bfloat16)
    return einsum("gstu,ugd->tgsd", weights, v).astype(jnp.bfloat16)


def reference(x, gain, wq, wk, wv, wo):
    a, place = normed(x, gain), jnp.arange(ROWS)
    q = turned(matmul(a, wq).reshape(ROWS, HEADS, HEAD), place, THETA).reshape(ROWS, KV_HEADS, -1, HEAD)
    k = turned(matmul(a, wk).reshape(ROWS, KV_HEADS, HEAD), place, THETA)
    v = matmul(a, wv).reshape(ROWS, KV_HEADS, HEAD)
    seen = attention(q, k, v).reshape(ROWS, HEADS * HEAD)
    return (x.astype(jnp.float32) + jnp.dot(seen, wo, preferred_element_type=jnp.float32)).astype(jnp.bfloat16)
```

```python
import jax
import jax.numpy as jnp
from jax import lax
from jax.experimental import pallas as pl
from jax.experimental.pallas import tpu as pltpu

NEG = -1e30
HIDDEN = 2 * NEG
LOG2E = 1.4426950408889634
VMEM = 60 * 2**20


def _dot(a, b, ca, cb):
    return lax.dot_general(a, b, (((ca,), (cb,)), ((), ())), preferred_element_type=jnp.float32)


from jax.sharding import PartitionSpec as P

HEAD = 256
THETA = 10000
Z = 4
MESH = pl.DeviceIdType.MESH


def normed(x, gain):
    wide = x.astype(jnp.float32)
    scale = lax.rsqrt(jnp.mean(wide * wide, -1, keepdims=True) + 1e-6)
    return (wide * scale * gain.astype(jnp.float32)).astype(jnp.bfloat16)


def _where():
    me = lax.axis_index("sp")
    return lax.axis_index("dp"), me // (2 * Z), (me // 2) % Z, me % 2


def _sp(y, z, c):
    return (y * Z + z) * 2 + c


def _send(src, dst, send_sem, recv_sem, device):
    copy = pltpu.make_async_remote_copy(src_ref=src, dst_ref=dst, send_sem=send_sem, recv_sem=recv_sem, device_id=device, device_id_type=MESH)
    return copy


def _meet(always, sometimes):
    barrier = pltpu.get_barrier_semaphore()
    count = len(always)
    for device in always:
        pl.semaphore_signal(barrier, inc=1, device_id=device, device_id_type=MESH)
    for there, device in sometimes:

        @pl.when(there)
        def _():
            pl.semaphore_signal(barrier, inc=1, device_id=device, device_id_type=MESH)

        count = count + there.astype(jnp.int32)
    pl.semaphore_wait(barrier, count)


PIECES = 4


def _project(a_ref, w_ref, freq_ref, q_ref, k_ref, v_ref, a_s, w_s, cos_s, sin_s, w_send, w_recv, a_send, a_recv):
    x, y, z, c = _where()
    me, h = _sp(y, z, c), 2 * y + c
    t, n = a_ref.shape[0], w_ref.shape[2]
    r = w_ref.shape[1]
    part = t // PIECES
    beside, across, corner, twin = (x, _sp(y, z, 1 - c)), (x, _sp(1 - y, z, c)), (x, _sp(1 - y, z, 1 - c)), (1 - x, me)
    ahead, behind = (x, _sp(y, jnp.minimum(z + 1, Z - 1), c)), (x, _sp(y, jnp.maximum(z - 1, 0), c))
    _meet([beside, across, corner, twin], [(z < Z - 1, ahead), (z > 0, behind)])

    def rows(d):
        return w_s.at[pl.ds(pl.multiple_of(d * r, 16), r), :]

    def piece(slot, p):
        return a_s.at[slot, pl.ds(p * part, part), :]

    def w_copy(kind, d, device, src=None):
        return _send(rows(d) if src is None else src, rows(d), w_send.at[kind, d], w_recv.at[d], device)

    def w_wait(d):
        w_copy(0, d, twin).wait_recv()

    def first_w(j):
        to = (h + j) % 4
        return _send(w_ref.at[to], rows(me), w_send.at[0, j], w_recv.at[me], (x, _sp(to // 2, z, to % 2)))

    def own_a(kind, p, device):
        return _send(a_ref.at[pl.ds(p * part, part), :], piece(h, p), a_send.at[kind, p], a_recv.at[h, p], device)

    def relay_a(p):
        slot = 2 * (1 - y) + c
        return _send(piece(slot, p), piece(slot, p), a_send.at[2, p], a_recv.at[slot, p], beside)

    for j in (1, 2, 3):
        first_w(j).start()
    for p in range(PIECES):
        own_a(0, p, beside).start()
    for p in range(PIECES):
        own_a(1, p, across).start()
    w_s[pl.ds(pl.multiple_of(me * r, 16), r), :] = w_ref[h]
    a_s[h] = a_ref[...]

    for yy in (0, 1):
        d = _sp(yy, z, x)
        mine = (c == x) & (y == yy)

        @pl.when(mine)
        def _():
            @pl.when(z < Z - 1)
            def _():
                w_copy(1, d, ahead, w_ref.at[h]).start()

            @pl.when(z > 0)
            def _():
                w_copy(2, d, behind, w_ref.at[h]).start()

        @pl.when(jnp.logical_not(mine))
        def _():
            w_wait(d)

            @pl.when(z < Z - 1)
            def _():
                w_copy(1, d, ahead).start()

            @pl.when(z > 0)
            def _():
                w_copy(2, d, behind).start()

    step = min(256, t)

    def turn(i, _):
        slot, at = i // (t // step), (i % (t // step)) * step
        token = ((slot // 2) * Z + z) * 2 * t + (slot % 2) * t + at + lax.broadcasted_iota(jnp.int32, (step, HEAD // 2), 0)
        angle = token.astype(jnp.float32) * freq_ref[...]
        cos_s[pl.ds(i * step, step), :] = jnp.cos(angle)
        sin_s[pl.ds(i * step, step), :] = jnp.sin(angle)

    lax.fori_loop(0, 4 * t // step, turn, None)

    for s in range(1, Z):
        for sign in (1, -1):
            source = z - sign * s
            there = (source >= 0) & (source < Z)
            on = z + sign

            @pl.when(there)
            def _():
                for yy in (0, 1):
                    d = _sp(yy, source, x)
                    w_wait(d)

                    @pl.when((on >= 0) & (on < Z))
                    def _():
                        w_copy(1 if sign > 0 else 2, d, ahead if sign > 0 else behind).start()

                    w_copy(3, d, twin).start()

        relay_wait = _send(piece(2 * (1 - y) + c, s - 1), piece(2 * (1 - y) + c, s - 1), a_send.at[1, s - 1], a_recv.at[2 * (1 - y) + c, s - 1], across)
        relay_wait.wait_recv()
        relay_a(s - 1).start()
    for s in range(1, Z):
        for yy in (0, 1):
            w_wait(_sp(yy, (z + s) % Z, 1 - x))
    for yy in (0, 1):

        @pl.when(jnp.logical_not((c == 1 - x) & (y == yy)))
        def _():
            w_wait(_sp(yy, z, 1 - x))

    def project(slot, at):
        got = jnp.dot(a_s[slot, pl.ds(at, step), :], w_s[...], preferred_element_type=jnp.float32)
        got = got.astype(jnp.bfloat16).astype(jnp.float32)
        here = pl.ds(slot * t + at, step)
        cos, sin = cos_s[here, :], sin_s[here, :]
        half = HEAD // 2

        def turned(i):
            u, w = got[:, i * HEAD : i * HEAD + half], got[:, i * HEAD + half : (i + 1) * HEAD]
            return jnp.concatenate([u * cos - w * sin, w * cos + u * sin], -1).astype(jnp.bfloat16)

        q_ref[slot * 2, pl.ds(at, step), :] = turned(0)
        q_ref[slot * 2 + 1, pl.ds(at, step), :] = turned(1)
        there = pl.ds(pl.multiple_of((slot % 2) * t + at, 128), step)
        k_ref[slot // 2, there, :] = turned(2)
        v_ref[slot // 2, :, there] = got[:, 3 * HEAD :].T.astype(jnp.bfloat16)

    for p in range(PIECES):
        _send(piece(2 * y + 1 - c, p), piece(2 * y + 1 - c, p), a_send.at[0, p], a_recv.at[2 * y + 1 - c, p], beside).wait_recv()
    per = t // step
    lax.fori_loop(0, 2 * per, lambda i, _: project(2 * y + i // per, (i % per) * step), None)
    last = 2 * (1 - y) + c
    for p in range(Z - 1, PIECES):
        _send(piece(last, p), piece(last, p), a_send.at[1, p], a_recv.at[last, p], across).wait_recv()
        relay_a(p).start()
    lax.fori_loop(0, per, lambda i, _: project(last, i * step), None)
    last = 2 * (1 - y) + 1 - c
    for p in range(PIECES):
        _send(piece(last, p), piece(last, p), a_send.at[2, p], a_recv.at[last, p], beside).wait_recv()
    lax.fori_loop(0, per, lambda i, _: project(last, i * step), None)

    for j in (1, 2, 3):
        first_w(j).wait_send()
    for p in range(PIECES):
        own_a(0, p, beside).wait_send()
        own_a(1, p, across).wait_send()
        relay_a(p).wait_send()
    for s in range(Z):
        for sign in (1, -1):
            if s == 0:
                source, there = z, jnp.bool_(True)
            else:
                source = z - sign * s
                there = (source >= 0) & (source < Z)
            on = z + sign

            @pl.when(there & (on >= 0) & (on < Z))
            def _():
                for yy in (0, 1):
                    w_copy(1 if sign > 0 else 2, _sp(yy, source, x), ahead if sign > 0 else behind).wait_send()

            if s:

                @pl.when(there)
                def _():
                    for yy in (0, 1):
                        w_copy(3, _sp(yy, source, x), twin).wait_send()


def project(a, w, freq):
    t, d = a.shape
    n = w.shape[2]
    vmem = pl.BlockSpec(memory_space=pltpu.VMEM)
    return pl.pallas_call(
        _project,
        out_shape=[
            jax.ShapeDtypeStruct((8, t, HEAD), jnp.bfloat16),
            jax.ShapeDtypeStruct((2, 2 * t, HEAD), jnp.bfloat16),
            jax.ShapeDtypeStruct((2, HEAD, 2 * t), jnp.bfloat16),
        ],
        in_specs=[vmem] * 3,
        out_specs=[vmem] * 3,
        scratch_shapes=[
            pltpu.VMEM((4, t, d), jnp.bfloat16),
            pltpu.VMEM((d, n), jnp.bfloat16),
            pltpu.VMEM((4 * t, HEAD // 2), jnp.float32),
            pltpu.VMEM((4 * t, HEAD // 2), jnp.float32),
            pltpu.SemaphoreType.DMA((4, 16)),
            pltpu.SemaphoreType.DMA((16,)),
            pltpu.SemaphoreType.DMA((3, PIECES)),
            pltpu.SemaphoreType.DMA((4, PIECES)),
        ],
        compiler_params=pltpu.CompilerParams(collective_id=0, has_side_effects=True, vmem_limit_bytes=VMEM),
        cost_estimate=pl.CostEstimate(flops=8 * t * d * n, bytes_accessed=8 * t * d, transcendentals=0),
    )(a, w, freq)


def _attention(q_ref, k_ref, v_ref, o_ref, k_s, v_s, top_s, mix_s, o_s, k_send, k_recv, v_send, v_recv, o_send, o_recv, o_own):
    x, y, z, c = _where()
    h = 2 * y + c
    t = q_ref.shape[1]
    e_scale = HEAD**-0.5 * LOG2E
    ahead, behind = (x, _sp(y, jnp.minimum(z + 1, Z - 1), c)), (x, _sp(y, jnp.maximum(z - 1, 0), c))
    mates = [(x, _sp(((h + j) % 4) // 2, z, (h + j) % 2)) for j in (1, 2, 3)]
    _meet(mates, [(z < Z - 1, ahead), (z > 0, behind)])

    def copies(source, e, way, own=False):
        to = (x, _sp(y, jnp.clip(z + 1 - 2 * way, 0, Z - 1), c))
        k_from, v_from = (k_ref.at[e], v_ref.at[e]) if own else (k_s.at[source, e], v_s.at[source, e])
        return (
            _send(k_from, k_s.at[source, e], k_send.at[way, source, e], k_recv.at[source, e], to),
            _send(v_from, v_s.at[source, e], v_send.at[way, source, e], v_recv.at[source, e], to),
        )

    for e in (0, 1):

        @pl.when(z < Z - 1)
        def _():
            for copy in copies(z, e, 0, own=True):
                copy.start()

        if e == 0:

            @pl.when(z > 0)
            def _():
                for copy in copies(z, e, 1, own=True):
                    copy.start()

    k_s[z] = k_ref[...]
    v_s[z] = v_ref[...]
    top_s[...] = jnp.full(top_s.shape, NEG, jnp.float32)
    mix_s[...] = jnp.zeros(mix_s.shape, jnp.float32)
    ones = jnp.ones((8, t), jnp.bfloat16)

    def block(source, e, j, strips, masked):
        here = pl.ds(pl.multiple_of(j * t, 128), t)
        keys = k_s[source, e, here, :]
        values = jnp.concatenate([v_s[source, e, :, here], ones], axis=0)
        scores = [_dot(keys, q_ref[i], 1, 1) for i in strips]
        weights, keeps = [], []
        for i, s in zip(strips, scores):
            if masked:
                ok = lax.broadcasted_iota(jnp.int32, (t, t), 1) >= lax.broadcasted_iota(jnp.int32, (t, t), 0)
                s = jnp.where(ok, s, HIDDEN)
            old = top_s[i]
            top = jnp.maximum(old, s.max(axis=0, keepdims=True))
            top_s[i] = top
            weights.append(jnp.exp2((s - top) * e_scale).astype(jnp.bfloat16))
            keeps.append(jnp.exp2((old - top) * e_scale))
        for i, p, keep in zip(strips, weights, keeps):
            mix_s[i] = mix_s[i] * keep + _dot(values, p, 1, 0)

    def full(source, e, g, j):
        block(source, e, j, [4 * g + i for i in range(4)], False)

    def diagonal(i, _):
        g, j = i // 2, i % 2
        block(z, g, j, [4 * g + 2 * j, 4 * g + 2 * j + 1], True)

    lax.fori_loop(0, 4, diagonal, None)
    lax.fori_loop(0, 2, lambda g, _: block(z, g, 0, [4 * g + 2, 4 * g + 3], False), None)

    def unit(i, _):
        s, kind = (i + 2) // 3, (i + 2) % 3
        sign = jnp.where(kind == 1, -1, 1)
        source = z - sign * s
        e = kind // 2
        there = (source >= 0) & (source < Z) & ((s > 0) | (kind == 2))
        e = jnp.where(s == 0, 0, e)

        @pl.when(there)
        def _():
            @pl.when(s > 0)
            def _():
                way = jnp.where(kind == 1, 1, 0)
                for copy in copies(source, e, way):
                    copy.wait_recv()
                on = z + sign

                @pl.when((on >= 0) & (on < Z))
                def _():
                    for copy in copies(source, e, way):
                        copy.start()

            first = jnp.where(kind == 0, 0, 1)
            lax.fori_loop(2 * first, 4, lambda u, _: full(source, e, u // 2, u % 2), None)

    lax.fori_loop(0, 3 * Z - 2, unit, None)

    def finish(s4, _):
        for n in (0, 1):
            i = 2 * s4 + n
            o_s[s4, :, n * HEAD : (n + 1) * HEAD] = (mix_s[i, :HEAD, :] * (1 / mix_s[i, HEAD : HEAD + 1, :])).T.astype(jnp.bfloat16)

    lax.fori_loop(0, 4, finish, None)

    columns = o_ref.at[:, pl.ds(pl.multiple_of(h * 2 * HEAD, 128), 2 * HEAD)]

    def result(j):
        to = (h + j) % 4
        return _send(o_s.at[to], columns, o_send.at[j], o_recv.at[h], (x, _sp(to // 2, z, to % 2)))

    for j in (1, 2, 3):
        result(j).start()
    local = pltpu.make_async_copy(o_s.at[h], columns, o_own)
    local.start()
    local.wait()
    for j in (1, 2, 3):
        other = (h + j) % 4
        theirs = o_ref.at[:, pl.ds(pl.multiple_of(other * 2 * HEAD, 128), 2 * HEAD)]
        _send(o_s.at[other], theirs, o_send.at[j], o_recv.at[other], mates[j - 1]).wait_recv()
    for j in (1, 2, 3):
        result(j).wait_send()
    for source in range(Z):
        for e in (0, 1):

            @pl.when((z < Z - 1) & (source <= z))
            def _():
                for copy in copies(source, e, 0):
                    copy.wait_send()

            if e == 0:

                @pl.when((z > 0) & (source >= z))
                def _():
                    for copy in copies(source, e, 1):
                        copy.wait_send()


def attention(q, k, v):
    t = q.shape[1]
    vmem = pl.BlockSpec(memory_space=pltpu.VMEM)
    return pl.pallas_call(
        _attention,
        out_shape=jax.ShapeDtypeStruct((t, 8 * HEAD), jnp.bfloat16),
        in_specs=[vmem] * 3,
        out_specs=pl.BlockSpec(memory_space=pl.ANY),
        scratch_shapes=[
            pltpu.VMEM((Z, 2, 2 * t, HEAD), jnp.bfloat16),
            pltpu.VMEM((Z, 2, HEAD, 2 * t), jnp.bfloat16),
            pltpu.VMEM((8, 1, t), jnp.float32),
            pltpu.VMEM((8, HEAD + 8, t), jnp.float32),
            pltpu.VMEM((4, t, 2 * HEAD), jnp.bfloat16),
            pltpu.SemaphoreType.DMA((2, Z, 2)),
            pltpu.SemaphoreType.DMA((Z, 2)),
            pltpu.SemaphoreType.DMA((2, Z, 2)),
            pltpu.SemaphoreType.DMA((Z, 2)),
            pltpu.SemaphoreType.DMA((4,)),
            pltpu.SemaphoreType.DMA((4,)),
            pltpu.SemaphoreType.DMA,
        ],
        compiler_params=pltpu.CompilerParams(collective_id=1, has_side_effects=True, vmem_limit_bytes=VMEM),
        cost_estimate=pl.CostEstimate(flops=8 * t * 16 * t * 4 * HEAD, bytes_accessed=16 * t * HEAD, transcendentals=0),
    )(q, k, v)


def solution(mesh):
    def step(x, gain, wq, wk, wv, wo):
        wo = lax.all_gather(wo, "sp", axis=0, tiled=True)
        r = wq.shape[0]
        w = jnp.concatenate([wq.reshape(r, 4, -1), wk.reshape(r, 4, -1), wv.reshape(r, 4, -1)], -1).transpose(1, 0, 2)
        half = HEAD // 2
        freq = (THETA ** (-jnp.arange(half, dtype=jnp.float32) / half))[None]
        q, k, v = project(normed(x, gain), w, freq)
        seen = attention(q, k, v)
        y = jnp.dot(seen, wo, preferred_element_type=jnp.float32)
        return (x.astype(jnp.float32) + y).astype(jnp.bfloat16)

    tokens, whole = P(("dp", "sp"), None), P("sp", None)
    return jax.shard_map(
        step,
        mesh=mesh,
        in_specs=(tokens, P(None), whole, whole, whole, whole),
        out_specs=tokens,
        check_vma=False,
    )
```

```python
import jax
import jax.numpy as jnp
import numpy as np
from jax import lax
from jax.experimental import pallas as pl
from jax.experimental.pallas import tpu as pltpu
from jax.sharding import PartitionSpec as P


NEG = -1e30
HIDDEN = 2 * NEG
LOG2E = 1.4426950408889634
VMEM = 67043328
HEAD = 256
THETA = 10000
Z = 4
PIECES = 4
MESH = pl.DeviceIdType.MESH


def _dot(a, b, ca, cb):
    return lax.dot_general(a, b, (((ca,), (cb,)), ((), ())), preferred_element_type=jnp.float32)


def _sp(y, z, c):
    return (y * Z + z) * 2 + c


def _send(src, dst, send_sem, recv_sem, device):
    return pltpu.make_async_remote_copy(src_ref=src, dst_ref=dst, send_sem=send_sem, recv_sem=recv_sem, device_id=device, device_id_type=MESH)


def _meet(always, sometimes):
    barrier = pltpu.get_barrier_semaphore()
    count = len(always)
    for device in always:
        pl.semaphore_signal(barrier, inc=1, device_id=device, device_id_type=MESH)
    for there, device in sometimes:

        @pl.when(there)
        def _():
            pl.semaphore_signal(barrier, inc=1, device_id=device, device_id_type=MESH)

        count = count + there.astype(jnp.int32)
    pl.semaphore_wait(barrier, count)


def _kernel(x_ref, gain_ref, wq_ref, wk_ref, wv_ref, wo_ref, freq_ref, y_ref, a_s, w_s, wo_s, cos_s, sin_s, q_s, k_s, v_s, top_s, mix_s, o_s, og_s,
            own_sem, w_first, w_send, w_recv, wo_send, wo_recv, a_send, a_recv, k_send, k_recv, v_send, v_recv, o_send, o_recv):
    x = lax.axis_index("dp")
    me = lax.axis_index("sp")
    y, z, c = me // (2 * Z), (me // 2) % Z, me % 2
    h = 2 * y + c
    t, r, ro = x_ref.shape[0], wq_ref.shape[0], wo_ref.shape[0]
    part = t // PIECES
    e_scale = HEAD**-0.5 * LOG2E
    beside, across, corner, twin = (x, _sp(y, z, 1 - c)), (x, _sp(1 - y, z, c)), (x, _sp(1 - y, z, 1 - c)), (1 - x, me)
    along = [(x, _sp(y, jnp.minimum(z + 1, Z - 1), c)), (x, _sp(y, jnp.maximum(z - 1, 0), c))]
    goes = [z < Z - 1, z > 0]
    _meet([beside, across, corner, twin], list(zip(goes, along)))

    def w_rows(d):
        return pl.ds(pl.multiple_of(d * r, 16), r)

    column = [0, 2 * HEAD, 3 * HEAD, 4 * HEAD]
    given = [wq_ref, wk_ref, wv_ref]

    def w_part(i, head):
        wide = column[i + 1] - column[i]
        return given[i].at[:, pl.ds(pl.multiple_of(head * wide, 128), wide)]

    def w_place(i, d):
        return w_s.at[w_rows(d), column[i] : column[i + 1]]

    def w_give(i, j):
        to = (h + j) % 4
        return _send(w_part(i, to), w_place(i, me), w_first.at[i, j], w_recv.at[i, me], (x, _sp(to // 2, z, to % 2)))

    def w_given(yy, cc):
        d = _sp(yy, z, cc)
        for i in range(3):
            _send(w_place(i, d), w_place(i, d), w_first.at[i, 0], w_recv.at[i, d], twin).wait_recv()

    def w_copy(kind, d):
        place = w_s.at[w_rows(d), :]
        return _send(place, place, w_send.at[kind, d], w_recv.at[0, d], twin if kind == 2 else along[kind])

    def own_w(i):
        return pltpu.make_async_copy(w_part(i, h), w_place(i, me), own_sem.at[i])

    def wo_copy(kind, d):
        place = wo_s.at[pl.ds(pl.multiple_of(d * ro, 16), ro), :]
        return _send(place, place, wo_send.at[kind, d], wo_recv.at[d], [along[0], along[1], twin, across, beside][kind])

    def own_wo():
        return pltpu.make_async_copy(wo_ref, wo_s.at[pl.ds(pl.multiple_of(me * ro, 16), ro), :], own_sem.at[3])

    def piece(slot, p):
        return a_s.at[slot, pl.ds(p * part, part), :]

    def a_copy(kind, slot, p):
        return _send(piece(slot, p), piece(slot, p), a_send.at[kind, p], a_recv.at[slot, p], across if kind == 1 else beside)

    over, diagonal_slot, beside_slot = 2 * (1 - y) + c, 2 * (1 - y) + 1 - c, 2 * y + 1 - c

    def relay_a(p):
        a_copy(1, over, p).wait_recv()
        a_copy(2, over, p).start()

    for j in (1, 2, 3):
        for i in (1, 2, 0):
            w_give(i, j).start()
    for i in range(3):
        own_w(i).start()
    own_wo().start()
    for p in range(PIECES):
        at = pl.ds(p * part, part)
        wide = x_ref[at, :].astype(jnp.float32)
        scale = lax.rsqrt(jnp.mean(wide * wide, -1, keepdims=True) + 1e-6)
        a_s[h, at, :] = (wide * scale * gain_ref[...].astype(jnp.float32)).astype(jnp.bfloat16)
        a_copy(1, h, p).start()
        a_copy(0, h, p).start()
    for i in range(3):
        own_w(i).wait()

    for yy in (0, 1):

        @pl.when(jnp.logical_not((c == x) & (y == yy)))
        def _():
            w_given(yy, x)

        for way in (0, 1):

            @pl.when(goes[way])
            def _():
                w_copy(way, _sp(yy, z, x)).start()

    step = min(256, t)

    def turn(i, _):
        slot, at = i // (t // step), (i % (t // step)) * step
        token = ((slot // 2) * Z + z) * 2 * t + (slot % 2) * t + at + lax.broadcasted_iota(jnp.int32, (step, HEAD // 2), 0)
        angle = token.astype(jnp.float32) * freq_ref[...]
        cos_s[pl.ds(i * step, step), :] = jnp.cos(angle)
        sin_s[pl.ds(i * step, step), :] = jnp.sin(angle)

    lax.fori_loop(0, 4 * t // step, turn, None)

    def arriving(s, way):
        source = z - s if way == 0 else z + s
        return source, (source >= 0) & (source < Z), goes[way]

    for s in range(1, Z):
        for way in (0, 1):
            source, there, on = arriving(s, way)

            @pl.when(there)
            def _():
                for yy in (0, 1):
                    w_copy(way, _sp(yy, source, x)).wait_recv()

                    @pl.when(on)
                    def _():
                        w_copy(way, _sp(yy, source, x)).start()

                    w_copy(2, _sp(yy, source, x)).start()

        relay_a(s - 1)
    own_wo().wait()

    @pl.when(c == x)
    def _():
        for way in (0, 1):

            @pl.when(goes[way])
            def _():
                wo_copy(way, me).start()

    def pass_wo(s):
        @pl.when(c == x)
        def _():
            for way in (0, 1):
                source, there, on = arriving(s, way)

                @pl.when(there)
                def _():
                    wo_copy(way, _sp(y, source, c)).wait_recv()

                    @pl.when(on)
                    def _():
                        wo_copy(way, _sp(y, source, c)).start()

                    wo_copy(2, _sp(y, source, c)).start()

    pass_wo(1)
    for yy in (0, 1):
        for s in range(1, Z):
            w_copy(2, _sp(yy, (z + s) % Z, 1 - x)).wait_recv()

        @pl.when(jnp.logical_not((c == 1 - x) & (y == yy)))
        def _():
            w_given(yy, 1 - x)

    half = HEAD // 2

    def turned(got, i, here):
        u, w = got[:, i * HEAD : i * HEAD + half], got[:, i * HEAD + half : (i + 1) * HEAD]
        cos, sin = cos_s[here, :], sin_s[here, :]
        return jnp.concatenate([u * cos - w * sin, w * cos + u * sin], -1).astype(jnp.bfloat16)

    def product(slot, at, columns):
        got = jnp.dot(a_s[slot, pl.ds(at, step), :], w_s[:, columns], preferred_element_type=jnp.float32)
        return got.astype(jnp.bfloat16).astype(jnp.float32)

    def keys_values(slot, at):
        got = product(slot, at, slice(2 * HEAD, 4 * HEAD))
        there = pl.ds(pl.multiple_of((slot % 2) * t + at, 128), step)
        k_s[z, slot // 2, there, :] = turned(got, 0, pl.ds(slot * t + at, step))
        v_s[z, slot // 2, :, there] = got[:, HEAD:].T.astype(jnp.bfloat16)

    def queries(slot, at):
        got = product(slot, at, slice(0, 2 * HEAD))
        for n in (0, 1):
            q_s[slot * 2 + n, pl.ds(at, step), :] = turned(got, n, pl.ds(slot * t + at, step))

    per = t // step

    def unit_copies(source, e, way):
        to = (x, _sp(y, jnp.clip(z + 1 - 2 * way, 0, Z - 1), c))
        k_at, v_at = k_s.at[source, e], v_s.at[source, e]
        return (
            _send(k_at, k_at, k_send.at[way, source, e], k_recv.at[source, e], to),
            _send(v_at, v_at, v_send.at[way, source, e], v_recv.at[source, e], to),
        )

    def give_unit(e):
        @pl.when(z < Z - 1)
        def _():
            for copy in unit_copies(z, e, 0):
                copy.start()

        @pl.when((z > 0) & (e == 0))
        def _():
            for copy in unit_copies(z, e, 1):
                copy.start()

    for p in range(PIECES):
        a_copy(0, beside_slot, p).wait_recv()
    lax.fori_loop(0, 2 * per, lambda i, _: keys_values(2 * y + i // per, (i % per) * step), None)
    give_unit(y)
    pass_wo(2)
    lax.fori_loop(0, 2 * per, lambda i, _: queries(2 * y + i // per, (i % per) * step), None)
    for p in range(Z - 1, PIECES):
        relay_a(p)
    lax.fori_loop(0, per, lambda i, _: keys_values(over, i * step), None)
    for p in range(PIECES):
        a_copy(2, diagonal_slot, p).wait_recv()
    lax.fori_loop(0, per, lambda i, _: keys_values(diagonal_slot, i * step), None)
    give_unit(1 - y)
    pass_wo(3)
    lax.fori_loop(0, 2 * per, lambda i, _: queries(2 * (1 - y) + i // per, (i % per) * step), None)

    for s in range(1, Z):

        @pl.when(c != x)
        def _():
            wo_copy(2, _sp(y, (z + s) % Z, c)).wait_recv()

    for zz in range(Z):
        wo_copy(3, _sp(y, zz, c)).start()
        wo_copy(4, _sp(y, zz, c)).start()

    top_s[...] = jnp.full(top_s.shape, NEG, jnp.float32)
    mix_s[...] = jnp.zeros(mix_s.shape, jnp.float32)
    ones = jnp.ones((8, t), jnp.bfloat16)

    def block(source, e, j, strips, masked):
        here = pl.ds(pl.multiple_of(j * t, 128), t)
        keys = k_s[source, e, here, :]
        values = jnp.concatenate([v_s[source, e, :, here], ones], axis=0)
        scores = [_dot(keys, q_s[i], 1, 1) for i in strips]
        weights, keeps = [], []
        for i, s in zip(strips, scores):
            if masked:
                ok = lax.broadcasted_iota(jnp.int32, (t, t), 1) >= lax.broadcasted_iota(jnp.int32, (t, t), 0)
                s = jnp.where(ok, s, HIDDEN)
            old = top_s[i]
            top = jnp.maximum(old, s.max(axis=0, keepdims=True))
            top_s[i] = top
            weights.append(jnp.exp2((s - top) * e_scale).astype(jnp.bfloat16))
            keeps.append(jnp.exp2((old - top) * e_scale))
        for i, p, keep in zip(strips, weights, keeps):
            mix_s[i] = mix_s[i] * keep + _dot(values, p, 1, 0)

    def full(source, e, g, j):
        block(source, e, j, [4 * g + i for i in range(4)], False)

    def diagonal(i, _):
        g, j = i // 2, i % 2
        block(z, g, j, [4 * g + 2 * j, 4 * g + 2 * j + 1], True)

    lax.fori_loop(0, 4, diagonal, None)
    lax.fori_loop(0, 2, lambda g, _: block(z, g, 0, [4 * g + 2, 4 * g + 3], False), None)

    def result(to):
        return _send(o_s.at[to], og_s.at[h], o_send.at[to], o_recv.at[h], (x, _sp(to // 2, z, to % 2)))

    def finish(g):
        def slot(i, _):
            s4 = 2 * g + i
            for n in (0, 1):
                o_s[s4, :, n * HEAD : (n + 1) * HEAD] = (mix_s[2 * s4 + n, :HEAD, :] * (1 / mix_s[2 * s4 + n, HEAD : HEAD + 1, :])).T.astype(jnp.bfloat16)

            @pl.when(s4 != h)
            def _():
                result(s4).start()

        lax.fori_loop(0, 2, slot, None)

    def unit(i, _):
        s, kind = (i + 2) // 3, (i + 2) % 3
        sign = jnp.where(kind == 1, -1, 1)
        source = z - sign * s
        e = jnp.where(s == 0, 0, kind // 2)
        there = (source >= 0) & (source < Z)

        @pl.when(there)
        def _():
            @pl.when(s > 0)
            def _():
                way = jnp.where(kind == 1, 1, 0)
                for copy in unit_copies(source, e, way):
                    copy.wait_recv()
                on = z + sign

                @pl.when((on >= 0) & (on < Z))
                def _():
                    for copy in unit_copies(source, e, way):
                        copy.start()

            first = jnp.where(kind == 0, 0, 1)
            lax.fori_loop(2 * first, 4, lambda u, _: full(source, e, u // 2, u % 2), None)

            @pl.when(((kind == 0) & (s == z)) | ((s == 0) & (z == 0)))
            def _():
                finish(0)

    lax.fori_loop(0, 3 * Z - 2, unit, None)
    for zz in range(Z):
        wo_copy(3, _sp(1 - y, zz, c)).wait_recv()
        wo_copy(4, _sp(1 - y, zz, c)).start()
    finish(1)

    for zz in range(Z):
        for yy in (0, 1):
            wo_copy(4, _sp(yy, zz, 1 - c)).wait_recv()

    og_s[h] = o_s[h]
    for j in (1, 2, 3):
        other = (h + j) % 4
        _send(og_s.at[other], og_s.at[other], o_send.at[other], o_recv.at[other], twin).wait_recv()
    wide = 256

    def output(i, _):
        at = pl.ds(pl.multiple_of(i * wide, 128), wide)
        total = x_ref[:, at].astype(jnp.float32)
        for n in range(4):
            total = total + jnp.dot(og_s[n], wo_s[n * 2 * HEAD : (n + 1) * 2 * HEAD, at], preferred_element_type=jnp.float32)
        y_ref[:, at] = total.astype(jnp.bfloat16)

    lax.fori_loop(0, x_ref.shape[1] // wide, output, None)

    for j in (1, 2, 3):
        for i in range(3):
            w_give(i, j).wait_send()
        result((h + j) % 4).wait_send()
    for p in range(PIECES):
        a_copy(0, h, p).wait_send()
        a_copy(1, h, p).wait_send()
        a_copy(2, over, p).wait_send()
    for s in range(Z):
        for way in (0, 1):
            source, there, on = arriving(s, way)

            @pl.when(there & on)
            def _():
                for yy in (0, 1):
                    w_copy(way, _sp(yy, source, x)).wait_send()

                @pl.when(c == x)
                def _():
                    wo_copy(way, _sp(y, source, c)).wait_send()

            if s:

                @pl.when(there)
                def _():
                    for yy in (0, 1):
                        w_copy(2, _sp(yy, source, x)).wait_send()

                    @pl.when(c == x)
                    def _():
                        wo_copy(2, _sp(y, source, c)).wait_send()

    for zz in range(Z):
        wo_copy(3, _sp(y, zz, c)).wait_send()
        wo_copy(4, _sp(y, zz, c)).wait_send()
        wo_copy(4, _sp(1 - y, zz, c)).wait_send()
    for source in range(Z):
        for e in (0, 1):

            @pl.when((z < Z - 1) & (source <= z))
            def _():
                for copy in unit_copies(source, e, 0):
                    copy.wait_send()

            if e == 0:

                @pl.when((z > 0) & (source >= z))
                def _():
                    for copy in unit_copies(source, e, 1):
                        copy.wait_send()


def solution(mesh):
    half = HEAD // 2
    freq = np.power(np.float32(THETA), -np.arange(half, dtype=np.float32) / np.float32(half)).astype(np.float32)[None]

    def step(x, gain, wq, wk, wv, wo):
        t, d = x.shape
        vmem, far = pl.BlockSpec(memory_space=pltpu.VMEM), pl.BlockSpec(memory_space=pl.ANY)
        low, dma = jnp.bfloat16, pltpu.SemaphoreType.DMA
        return pl.pallas_call(
            _kernel,
            out_shape=jax.ShapeDtypeStruct((t, d), low),
            in_specs=[vmem, vmem, far, far, far, far, vmem],
            out_specs=vmem,
            scratch_shapes=[
                pltpu.VMEM((4, t, d), low),
                pltpu.VMEM((d, 4 * HEAD), low),
                pltpu.VMEM((8 * HEAD, d), low),
                pltpu.VMEM((4 * t, half), jnp.float32),
                pltpu.VMEM((4 * t, half), jnp.float32),
                pltpu.VMEM((8, t, HEAD), low),
                pltpu.VMEM((Z, 2, 2 * t, HEAD), low),
                pltpu.VMEM((Z, 2, HEAD, 2 * t), low),
                pltpu.VMEM((8, 1, t), jnp.float32),
                pltpu.VMEM((8, HEAD + 8, t), jnp.float32),
                pltpu.VMEM((4, t, 2 * HEAD), low),
                pltpu.VMEM((4, t, 2 * HEAD), low),
                dma((4,)),
                dma((3, 4)),
                dma((3, 16)),
                dma((3, 16)),
                dma((5, 16)),
                dma((16,)),
                dma((3, PIECES)),
                dma((4, PIECES)),
                dma((2, Z, 2)),
                dma((Z, 2)),
                dma((2, Z, 2)),
                dma((Z, 2)),
                dma((4,)),
                dma((4,)),
            ],
            compiler_params=pltpu.CompilerParams(collective_id=0, has_side_effects=True, vmem_limit_bytes=VMEM),
            cost_estimate=pl.CostEstimate(flops=2 * t * d * 6144 + 8 * t * 16 * t * 4 * HEAD, bytes_accessed=48 * 2**20, transcendentals=0),
        )(x, gain[None], wq, wk, wv, wo, jnp.asarray(freq))

    tokens, whole = P(("dp", "sp"), None), P("sp", None)
    return jax.shard_map(
        step,
        mesh=mesh,
        in_specs=(tokens, P(None), whole, whole, whole, whole),
        out_specs=tokens,
        check_vma=False,
    )
```

```python
import jax
import jax.numpy as jnp
import numpy as np
from jax import lax
from jax.experimental import pallas as pl
from jax.experimental.pallas import tpu as pltpu
from jax.sharding import PartitionSpec as P


NEG = -1e30
HIDDEN = 2 * NEG
LOG2E = 1.4426950408889634
VMEM = 67043328
HEAD = 256
THETA = 10000
Z = 4
PIECES = 4
MESH = pl.DeviceIdType.MESH


def _dot(a, b, ca, cb):
    return lax.dot_general(a, b, (((ca,), (cb,)), ((), ())), preferred_element_type=jnp.float32)


def _sp(y, z, c):
    return (y * Z + z) * 2 + c


def _send(src, dst, send_sem, recv_sem, device):
    return pltpu.make_async_remote_copy(src_ref=src, dst_ref=dst, send_sem=send_sem, recv_sem=recv_sem, device_id=device, device_id_type=MESH)


def _meet(always, sometimes):
    barrier = pltpu.get_barrier_semaphore()
    count = len(always)
    for device in always:
        pl.semaphore_signal(barrier, inc=1, device_id=device, device_id_type=MESH)
    for there, device in sometimes:

        @pl.when(there)
        def _():
            pl.semaphore_signal(barrier, inc=1, device_id=device, device_id_type=MESH)

        count = count + there.astype(jnp.int32)
    pl.semaphore_wait(barrier, count)


def _kernel(x_ref, gain_ref, wq_ref, wk_ref, wv_ref, wo_ref, freq_ref, y_ref, a_s, w_s, wo_s, cos_s, sin_s, q_s, k_s, v_s, top_s, mix_s, o_s, og_s, part_s, stat_s,
            own_sem, w_first, w_send, w_recv, wo_send, wo_recv, a_send, a_recv, k_send, k_recv, v_send, v_recv, o_send, o_recv, help_send, help_recv):
    x = lax.axis_index("dp")
    me = lax.axis_index("sp")
    y, z, c = me // (2 * Z), (me // 2) % Z, me % 2
    h = 2 * y + c
    t, r, ro = x_ref.shape[0], wq_ref.shape[0], wo_ref.shape[0]
    part = t // PIECES
    e_scale = HEAD**-0.5 * LOG2E
    beside, across, corner, twin = (x, _sp(y, z, 1 - c)), (x, _sp(1 - y, z, c)), (x, _sp(1 - y, z, 1 - c)), (1 - x, me)
    along = [(x, _sp(y, jnp.minimum(z + 1, Z - 1), c)), (x, _sp(y, jnp.maximum(z - 1, 0), c))]
    goes = [z < Z - 1, z > 0]
    _meet([beside, across, corner, twin], list(zip(goes, along)))

    def w_rows(d):
        return pl.ds(pl.multiple_of(d * r, 16), r)

    column = [0, 2 * HEAD, 3 * HEAD, 4 * HEAD]
    given = [wq_ref, wk_ref, wv_ref]

    def w_part(i, head):
        wide = column[i + 1] - column[i]
        return given[i].at[:, pl.ds(pl.multiple_of(head * wide, 128), wide)]

    def w_place(i, d):
        return w_s.at[w_rows(d), column[i] : column[i + 1]]

    def w_give(i, j):
        to = (h + j) % 4
        return _send(w_part(i, to), w_place(i, me), w_first.at[i, j], w_recv.at[i, me], (x, _sp(to // 2, z, to % 2)))

    def w_given(yy, cc, which):
        d = _sp(yy, z, cc)
        for i in (1, 2) if which else (0,):
            _send(w_place(i, d), w_place(i, d), w_first.at[i, 0], w_recv.at[i, d], twin).wait_recv()

    def w_copy(kind, d, which):
        place = w_s.at[w_rows(d), 2 * HEAD * which : 2 * HEAD * (which + 1)]
        return _send(place, place, w_send.at[kind, which, d], w_recv.at[which, d], twin if kind == 2 else along[kind])

    def own_w(i):
        return pltpu.make_async_copy(w_part(i, h), w_place(i, me), own_sem.at[i])

    def wo_copy(kind, d):
        place = wo_s.at[pl.ds(pl.multiple_of(d * ro, 16), ro), :]
        return _send(place, place, wo_send.at[kind, d], wo_recv.at[d], [along[0], along[1], twin, across, beside][kind])

    def own_wo():
        return pltpu.make_async_copy(wo_ref, wo_s.at[pl.ds(pl.multiple_of(me * ro, 16), ro), :], own_sem.at[3])

    def piece(slot, p):
        return a_s.at[slot, pl.ds(p * part, part), :]

    def a_copy(kind, slot, p):
        return _send(piece(slot, p), piece(slot, p), a_send.at[kind, p], a_recv.at[slot, p], across if kind == 1 else beside)

    over, diagonal_slot, beside_slot = 2 * (1 - y) + c, 2 * (1 - y) + 1 - c, 2 * y + 1 - c

    def relay_a(p):
        a_copy(1, over, p).wait_recv()
        a_copy(2, over, p).start()

    for which in (1, 0):
        for j in (1, 2, 3):
            for i in (1, 2) if which else (0,):
                w_give(i, j).start()
    for i in (1, 2, 0):
        own_w(i).start()
    own_wo().start()
    for p in range(PIECES):
        at = pl.ds(p * part, part)
        wide = x_ref[at, :].astype(jnp.float32)
        scale = lax.rsqrt(jnp.mean(wide * wide, -1, keepdims=True) + 1e-6)
        a_s[h, at, :] = (wide * scale * gain_ref[...].astype(jnp.float32)).astype(jnp.bfloat16)
        a_copy(1, h, p).start()
        a_copy(0, h, p).start()
    for i in range(3):
        own_w(i).wait()

    def give_w(which):
        for yy in (0, 1):

            @pl.when(jnp.logical_not((c == x) & (y == yy)))
            def _():
                w_given(yy, x, which)

            for way in (0, 1):

                @pl.when(goes[way])
                def _():
                    w_copy(way, _sp(yy, z, x), which).start()

    def arriving(s, way):
        source = z - s if way == 0 else z + s
        return source, (source >= 0) & (source < Z), goes[way]

    def pass_w(s, which):
        for way in (0, 1):
            source, there, on = arriving(s, way)

            @pl.when(there)
            def _():
                for yy in (0, 1):
                    w_copy(way, _sp(yy, source, x), which).wait_recv()

                    @pl.when(on)
                    def _():
                        w_copy(way, _sp(yy, source, x), which).start()

                    w_copy(2, _sp(yy, source, x), which).start()

    def w_rest(which):
        for yy in (0, 1):
            for s in range(1, Z):
                w_copy(2, _sp(yy, (z + s) % Z, 1 - x), which).wait_recv()

            @pl.when(jnp.logical_not((c == 1 - x) & (y == yy)))
            def _():
                w_given(yy, 1 - x, which)

    def pass_wo(s):
        @pl.when(c == x)
        def _():
            for way in (0, 1):
                source, there, on = arriving(s, way)

                @pl.when(there)
                def _():
                    wo_copy(way, _sp(y, source, c)).wait_recv()

                    @pl.when(on)
                    def _():
                        wo_copy(way, _sp(y, source, c)).start()

                    wo_copy(2, _sp(y, source, c)).start()

    give_w(1)

    step = min(256, t)

    def turn(i, _):
        slot, at = i // (t // step), (i % (t // step)) * step
        token = ((slot // 2) * Z + z) * 2 * t + (slot % 2) * t + at + lax.broadcasted_iota(jnp.int32, (step, HEAD // 2), 0)
        angle = token.astype(jnp.float32) * freq_ref[...]
        cos_s[pl.ds(i * step, step), :] = jnp.cos(angle)
        sin_s[pl.ds(i * step, step), :] = jnp.sin(angle)

    lax.fori_loop(0, 4 * t // step, turn, None)
    for s in range(1, Z):
        pass_w(s, 1)
    give_w(0)
    w_rest(1)

    half = HEAD // 2

    def turned(got, i, here):
        u, w = got[:, i * HEAD : i * HEAD + half], got[:, i * HEAD + half : (i + 1) * HEAD]
        cos, sin = cos_s[here, :], sin_s[here, :]
        return jnp.concatenate([u * cos - w * sin, w * cos + u * sin], -1).astype(jnp.bfloat16)

    def product(slot, at, columns):
        got = jnp.dot(a_s[slot, pl.ds(at, step), :], w_s[:, columns], preferred_element_type=jnp.float32)
        return got.astype(jnp.bfloat16).astype(jnp.float32)

    def keys_values(slot, at):
        got = product(slot, at, slice(2 * HEAD, 4 * HEAD))
        there = pl.ds(pl.multiple_of((slot % 2) * t + at, 128), step)
        k_s[z, slot // 2, there, :] = turned(got, 0, pl.ds(slot * t + at, step))
        v_s[z, slot // 2, :, there] = got[:, HEAD:].T.astype(jnp.bfloat16)

    def queries(slot, at):
        got = product(slot, at, slice(0, 2 * HEAD))
        for n in (0, 1):
            q_s[slot * 2 + n, pl.ds(at, step), :] = turned(got, n, pl.ds(slot * t + at, step))

    per = t // step

    def unit_copies(source, e, way):
        to = (x, _sp(y, jnp.clip(z + 1 - 2 * way, 0, Z - 1), c))
        k_at, v_at = k_s.at[source, e], v_s.at[source, e]
        return (
            _send(k_at, k_at, k_send.at[way, source, e], k_recv.at[source, e], to),
            _send(v_at, v_at, v_send.at[way, source, e], v_recv.at[source, e], to),
        )

    def give_unit(e):
        @pl.when(z < Z - 1 - e)
        def _():
            for copy in unit_copies(z, e, 0):
                copy.start()

        @pl.when((z > 0) & (e == 0))
        def _():
            for copy in unit_copies(z, e, 1):
                copy.start()

    for p in range(PIECES):
        a_copy(0, beside_slot, p).wait_recv()
    lax.fori_loop(0, 2 * per, lambda i, _: keys_values(2 * y + i // per, (i % per) * step), None)
    for s in range(1, Z):
        pass_w(s, 0)
    give_unit(y)
    own_wo().wait()

    @pl.when(c == x)
    def _():
        for way in (0, 1):

            @pl.when(goes[way])
            def _():
                wo_copy(way, me).start()

    w_rest(0)
    lax.fori_loop(0, 2 * per, lambda i, _: queries(2 * y + i // per, (i % per) * step), None)
    for p in range(PIECES):
        relay_a(p)
    lax.fori_loop(0, per, lambda i, _: keys_values(over, i * step), None)
    for p in range(PIECES):
        a_copy(2, diagonal_slot, p).wait_recv()
    lax.fori_loop(0, per, lambda i, _: keys_values(diagonal_slot, i * step), None)
    pass_wo(1)
    give_unit(1 - y)
    lax.fori_loop(0, 2 * per, lambda i, _: queries(2 * (1 - y) + i // per, (i % per) * step), None)

    def help_copy(i):
        if i == 0:
            return _send(q_s.at[4:8], q_s.at[8:12], help_send.at[0], help_recv.at[0], along[1])
        place = part_s if i == 1 else stat_s
        return _send(place, place, help_send.at[i], help_recv.at[i], along[0])

    helps, helped = z == Z - 2, z == Z - 1

    @pl.when(helped)
    def _():
        help_copy(0).start()

    pass_wo(2)

    top_s[...] = jnp.full(top_s.shape, NEG, jnp.float32)
    mix_s[...] = jnp.zeros(mix_s.shape, jnp.float32)
    ones = jnp.ones((8, t), jnp.bfloat16)

    def block(source, e, j, strips, masked):
        here = pl.ds(pl.multiple_of(j * t, 128), t)
        keys = k_s[source, e, here, :]
        values = jnp.concatenate([v_s[source, e, :, here], ones], axis=0)
        scores = [_dot(keys, q_s[i], 1, 1) for i in strips]
        weights, keeps = [], []
        for i, s in zip(strips, scores):
            if masked:
                ok = lax.broadcasted_iota(jnp.int32, (t, t), 1) >= lax.broadcasted_iota(jnp.int32, (t, t), 0)
                s = jnp.where(ok, s, HIDDEN)
            old = top_s[i]
            top = jnp.maximum(old, s.max(axis=0, keepdims=True))
            top_s[i] = top
            weights.append(jnp.exp2((s - top) * e_scale).astype(jnp.bfloat16))
            keeps.append(jnp.exp2((old - top) * e_scale))
        for i, p, keep in zip(strips, weights, keeps):
            mix_s[i] = mix_s[i] * keep + _dot(values, p, 1, 0)

    def full(source, e, g, j):
        block(source, e, j, [4 * g + i for i in range(4)], False)

    def diagonal(i, _):
        g, j = i // 2, i % 2
        block(z, g, j, [4 * g + 2 * j, 4 * g + 2 * j + 1], True)

    lax.fori_loop(0, 4, diagonal, None)
    lax.fori_loop(0, 2, lambda g, _: block(z, g, 0, [4 * g + 2, 4 * g + 3], False), None)

    def result(to):
        return _send(o_s.at[to], og_s.at[h], o_send.at[to], o_recv.at[h], (x, _sp(to // 2, z, to % 2)))

    def finish(g):
        def slot(i, _):
            s4 = 2 * g + i
            for n in (0, 1):
                o_s[s4, :, n * HEAD : (n + 1) * HEAD] = (mix_s[2 * s4 + n, :HEAD, :] * (1 / mix_s[2 * s4 + n, HEAD : HEAD + 1, :])).T.astype(jnp.bfloat16)

            @pl.when(s4 != h)
            def _():
                result(s4).start()

        lax.fori_loop(0, 2, slot, None)

    def finish_help():
        for n in range(4):
            i = 8 + n
            total = mix_s[i, HEAD : HEAD + 1, :]
            part_s[n] = (mix_s[i, :HEAD, :] * (1 / total)).astype(jnp.bfloat16)
            stat_s[n, 0:1, :] = top_s[i]
            stat_s[n, 1:2, :] = total
        help_copy(1).start()
        help_copy(2).start()

    def take_help():
        for n in range(4):
            i = 4 + n
            old, new = top_s[i], stat_s[n, 0:1, :]
            top = jnp.maximum(old, new)
            keep, gain = jnp.exp2((old - top) * e_scale), jnp.exp2((new - top) * e_scale) * stat_s[n, 1:2, :]
            mix_s[i, :HEAD, :] = mix_s[i, :HEAD, :] * keep + part_s[n].astype(jnp.float32) * gain
            mix_s[i, HEAD:, :] = mix_s[i, HEAD:, :] * keep + gain

    def unit(i, _):
        s, kind = (i + 2) // 3, (i + 2) % 3
        sign = jnp.where(kind == 1, -1, 1)
        source = z - sign * s
        e = jnp.where(s == 0, 0, kind // 2)
        there = (source >= 0) & (source < Z) & ((e == 0) | jnp.logical_not(helped))
        both = helps & (e == 1)
        extra = jnp.where(both & (s == 1), 2, 0)

        @pl.when(there)
        def _():
            @pl.when(s > 0)
            def _():
                way = jnp.where(kind == 1, 1, 0)
                for copy in unit_copies(source, e, way):
                    copy.wait_recv()
                on = z + sign

                @pl.when((on >= 0) & (on < Z - e))
                def _():
                    for copy in unit_copies(source, e, way):
                        copy.start()

            @pl.when(extra > 0)
            def _():
                help_copy(0).wait_recv()

            most = jnp.where(both, 2, 1)
            rounds = 2 * (most + 1 - jnp.where(kind == 0, 0, 1)) + extra

            def work(u, _):
                own = u < extra
                full(jnp.where(own, z, source), e, jnp.where(own, 2, most - (u - extra) // 2), u % 2)

                @pl.when(both & (s == Z - 2) & (u == 1))
                def _():
                    finish_help()

            lax.fori_loop(0, rounds, work, None)

            @pl.when(((kind == 0) & (s == z)) | ((s == 0) & (z == 0)))
            def _():
                finish(0)

    lax.fori_loop(0, 4, unit, None)

    pass_wo(3)
    for s in range(1, Z):

        @pl.when(c != x)
        def _():
            wo_copy(2, _sp(y, (z + s) % Z, c)).wait_recv()

    for zz in range(Z):
        wo_copy(3, _sp(y, zz, c)).start()
        wo_copy(4, _sp(y, zz, c)).start()
    lax.fori_loop(4, 3 * Z - 2, unit, None)

    @pl.when(helped)
    def _():
        help_copy(1).wait_recv()
        help_copy(2).wait_recv()
        take_help()

    finish(1)
    for zz in range(Z):
        wo_copy(3, _sp(1 - y, zz, c)).wait_recv()
        wo_copy(4, _sp(1 - y, zz, c)).start()

    for zz in range(Z):
        for yy in (0, 1):
            wo_copy(4, _sp(yy, zz, 1 - c)).wait_recv()

    og_s[h] = o_s[h]
    for j in (1, 2, 3):
        other = (h + j) % 4
        _send(og_s.at[other], og_s.at[other], o_send.at[other], o_recv.at[other], twin).wait_recv()
    wide = 256

    def output(i, _):
        at = pl.ds(pl.multiple_of(i * wide, 128), wide)
        total = x_ref[:, at].astype(jnp.float32)
        for n in range(4):
            total = total + jnp.dot(og_s[n], wo_s[n * 2 * HEAD : (n + 1) * 2 * HEAD, at], preferred_element_type=jnp.float32)
        y_ref[:, at] = total.astype(jnp.bfloat16)

    lax.fori_loop(0, x_ref.shape[1] // wide, output, None)

    for j in (1, 2, 3):
        for i in range(3):
            w_give(i, j).wait_send()
        result((h + j) % 4).wait_send()
    for p in range(PIECES):
        a_copy(0, h, p).wait_send()
        a_copy(1, h, p).wait_send()
        a_copy(2, over, p).wait_send()
    for s in range(Z):
        for way in (0, 1):
            source, there, on = arriving(s, way)

            @pl.when(there & on)
            def _():
                for yy in (0, 1):
                    for which in (0, 1):
                        w_copy(way, _sp(yy, source, x), which).wait_send()

                @pl.when(c == x)
                def _():
                    wo_copy(way, _sp(y, source, c)).wait_send()

            if s:

                @pl.when(there)
                def _():
                    for yy in (0, 1):
                        for which in (0, 1):
                            w_copy(2, _sp(yy, source, x), which).wait_send()

                    @pl.when(c == x)
                    def _():
                        wo_copy(2, _sp(y, source, c)).wait_send()

    for zz in range(Z):
        wo_copy(3, _sp(y, zz, c)).wait_send()
        wo_copy(4, _sp(y, zz, c)).wait_send()
        wo_copy(4, _sp(1 - y, zz, c)).wait_send()
    @pl.when(helped)
    def _():
        help_copy(0).wait_send()

    @pl.when(helps)
    def _():
        help_copy(1).wait_send()
        help_copy(2).wait_send()

    for source in range(Z):
        for e in (0, 1):

            @pl.when((z < Z - 1 - e) & (source <= z))
            def _():
                for copy in unit_copies(source, e, 0):
                    copy.wait_send()

            if e == 0:

                @pl.when((z > 0) & (source >= z))
                def _():
                    for copy in unit_copies(source, e, 1):
                        copy.wait_send()


def solution(mesh):
    half = HEAD // 2
    freq = np.power(np.float32(THETA), -np.arange(half, dtype=np.float32) / np.float32(half)).astype(np.float32)[None]

    def step(x, gain, wq, wk, wv, wo):
        t, d = x.shape
        vmem, far = pl.BlockSpec(memory_space=pltpu.VMEM), pl.BlockSpec(memory_space=pl.ANY)
        low, dma = jnp.bfloat16, pltpu.SemaphoreType.DMA
        return pl.pallas_call(
            _kernel,
            out_shape=jax.ShapeDtypeStruct((t, d), low),
            in_specs=[vmem, vmem, far, far, far, far, vmem],
            out_specs=vmem,
            scratch_shapes=[
                pltpu.VMEM((4, t, d), low),
                pltpu.VMEM((d, 4 * HEAD), low),
                pltpu.VMEM((8 * HEAD, d), low),
                pltpu.VMEM((4 * t, half), jnp.float32),
                pltpu.VMEM((4 * t, half), jnp.float32),
                pltpu.VMEM((12, t, HEAD), low),
                pltpu.VMEM((Z, 2, 2 * t, HEAD), low),
                pltpu.VMEM((Z, 2, HEAD, 2 * t), low),
                pltpu.VMEM((12, 1, t), jnp.float32),
                pltpu.VMEM((12, HEAD + 8, t), jnp.float32),
                pltpu.VMEM((4, t, 2 * HEAD), low),
                pltpu.VMEM((4, t, 2 * HEAD), low),
                pltpu.VMEM((4, HEAD, t), low),
                pltpu.VMEM((4, 8, t), jnp.float32),
                dma((4,)),
                dma((3, 4)),
                dma((3, 2, 16)),
                dma((3, 16)),
                dma((5, 16)),
                dma((16,)),
                dma((3, PIECES)),
                dma((4, PIECES)),
                dma((2, Z, 2)),
                dma((Z, 2)),
                dma((2, Z, 2)),
                dma((Z, 2)),
                dma((4,)),
                dma((4,)),
                dma((3,)),
                dma((3,)),
            ],
            compiler_params=pltpu.CompilerParams(collective_id=0, has_side_effects=True, vmem_limit_bytes=VMEM),
            cost_estimate=pl.CostEstimate(flops=2 * t * d * 6144 + 8 * t * 16 * t * 4 * HEAD, bytes_accessed=48 * 2**20, transcendentals=0),
        )(x, gain[None], wq, wk, wv, wo, jnp.asarray(freq))

    tokens, whole = P(("dp", "sp"), None), P("sp", None)
    return jax.shard_map(
        step,
        mesh=mesh,
        in_specs=(tokens, P(None), whole, whole, whole, whole),
        out_specs=tokens,
        check_vma=False,
    )
```

```python
import jax
import jax.numpy as jnp
import numpy as np
from jax import lax
from jax.experimental import pallas as pl
from jax.experimental.pallas import tpu as pltpu
from jax.sharding import PartitionSpec as P


NEG = -1e30
HIDDEN = 2 * NEG
LOG2E = 1.4426950408889634
VMEM = 67043328
HEAD = 256
THETA = 10000
Z = 4
PIECES = 4
MESH = pl.DeviceIdType.MESH


def _dot(a, b, ca, cb):
    return lax.dot_general(a, b, (((ca,), (cb,)), ((), ())), preferred_element_type=jnp.float32)


def _sp(y, z, c):
    return (y * Z + z) * 2 + c


def _send(src, dst, send_sem, recv_sem, device):
    return pltpu.make_async_remote_copy(src_ref=src, dst_ref=dst, send_sem=send_sem, recv_sem=recv_sem, device_id=device, device_id_type=MESH)


def _meet(always, sometimes):
    barrier = pltpu.get_barrier_semaphore()
    count = len(always)
    for device in always:
        pl.semaphore_signal(barrier, inc=1, device_id=device, device_id_type=MESH)
    for there, device in sometimes:

        @pl.when(there)
        def _():
            pl.semaphore_signal(barrier, inc=1, device_id=device, device_id_type=MESH)

        count = count + there.astype(jnp.int32)
    pl.semaphore_wait(barrier, count)


def _kernel(x_ref, gain_ref, wq_ref, wk_ref, wv_ref, wo_ref, freq_ref, y_ref, a_s, w_s, wo_s, cos_s, sin_s, q_s, k_s, v_s, top_s, mix_s, o_s, og_s, part_s, stat_s, help_s,
            own_sem, w_first, w_send, w_recv, wo_send, wo_recv, a_send, a_recv, k_send, k_recv, v_send, v_recv, o_send, o_recv, help_send, help_recv):
    x = lax.axis_index("dp")
    me = lax.axis_index("sp")
    y, z, c = me // (2 * Z), (me // 2) % Z, me % 2
    h = 2 * y + c
    t, r, ro = x_ref.shape[0], wq_ref.shape[0], wo_ref.shape[0]
    part = t // PIECES
    e_scale = HEAD**-0.5 * LOG2E
    beside, across, corner, twin = (x, _sp(y, z, 1 - c)), (x, _sp(1 - y, z, c)), (x, _sp(1 - y, z, 1 - c)), (1 - x, me)
    along = [(x, _sp(y, jnp.minimum(z + 1, Z - 1), c)), (x, _sp(y, jnp.maximum(z - 1, 0), c))]
    goes = [z < Z - 1, z > 0]
    helps, helped = z == Z - 2, z == Z - 1
    taker, served = [(x, _sp(1, Z - 1, cc)) for cc in (0, 1)], helped & (y == 1)
    _meet([beside, across, corner, twin], list(zip(goes, along)) + [(helps, device) for device in taker]
          + [(served, (x, _sp(yy, Z - 2, cc))) for yy in (0, 1) for cc in (0, 1)])

    def w_rows(d):
        return pl.ds(pl.multiple_of(d * r, 16), r)

    column = [0, 2 * HEAD, 3 * HEAD, 4 * HEAD]
    given = [wq_ref, wk_ref, wv_ref]

    def w_part(i, head):
        wide = column[i + 1] - column[i]
        return given[i].at[:, pl.ds(pl.multiple_of(head * wide, 128), wide)]

    def w_place(i, d):
        return w_s.at[w_rows(d), column[i] : column[i + 1]]

    def w_give(i, j):
        to = (h + j) % 4
        return _send(w_part(i, to), w_place(i, me), w_first.at[i, j], w_recv.at[i, me], (x, _sp(to // 2, z, to % 2)))

    def w_given(yy, cc, which):
        d = _sp(yy, z, cc)
        for i in (1, 2) if which else (0,):
            _send(w_place(i, d), w_place(i, d), w_first.at[i, 0], w_recv.at[i, d], twin).wait_recv()

    def w_copy(kind, d, which):
        place = w_s.at[w_rows(d), 2 * HEAD * which : 2 * HEAD * (which + 1)]
        return _send(place, place, w_send.at[kind, which, d], w_recv.at[which, d], twin if kind == 2 else along[kind])

    def own_w(i):
        return pltpu.make_async_copy(w_part(i, h), w_place(i, me), own_sem.at[i])

    def wo_copy(kind, d):
        place = wo_s.at[pl.ds(pl.multiple_of(d * ro, 16), ro), :]
        return _send(place, place, wo_send.at[kind, d], wo_recv.at[d], [along[0], along[1], twin, across, beside][kind])

    def own_wo():
        return pltpu.make_async_copy(wo_ref, wo_s.at[pl.ds(pl.multiple_of(me * ro, 16), ro), :], own_sem.at[3])

    def piece(slot, p):
        return a_s.at[slot, pl.ds(p * part, part), :]

    def a_copy(kind, slot, p):
        return _send(piece(slot, p), piece(slot, p), a_send.at[kind, p], a_recv.at[slot, p], across if kind == 1 else beside)

    over, diagonal_slot, beside_slot = 2 * (1 - y) + c, 2 * (1 - y) + 1 - c, 2 * y + 1 - c

    def relay_a(p):
        a_copy(1, over, p).wait_recv()
        a_copy(2, over, p).start()

    for which in (1, 0):
        for j in (1, 2, 3):
            for i in (1, 2) if which else (0,):
                w_give(i, j).start()
    for i in (1, 2, 0):
        own_w(i).start()
    own_wo().start()
    for p in range(PIECES):
        at = pl.ds(p * part, part)
        wide = x_ref[at, :].astype(jnp.float32)
        scale = lax.rsqrt(jnp.mean(wide * wide, -1, keepdims=True) + 1e-6)
        a_s[h, at, :] = (wide * scale * gain_ref[...].astype(jnp.float32)).astype(jnp.bfloat16)
        a_copy(1, h, p).start()
        a_copy(0, h, p).start()
    for i in range(3):
        own_w(i).wait()

    def give_w(which):
        for yy in (0, 1):

            @pl.when(jnp.logical_not((c == x) & (y == yy)))
            def _():
                w_given(yy, x, which)

            for way in (0, 1):

                @pl.when(goes[way])
                def _():
                    w_copy(way, _sp(yy, z, x), which).start()

    def arriving(s, way):
        source = z - s if way == 0 else z + s
        return source, (source >= 0) & (source < Z), goes[way]

    def pass_w(s, which):
        for way in (0, 1):
            source, there, on = arriving(s, way)

            @pl.when(there)
            def _():
                for yy in (0, 1):
                    w_copy(way, _sp(yy, source, x), which).wait_recv()

                    @pl.when(on)
                    def _():
                        w_copy(way, _sp(yy, source, x), which).start()

                    w_copy(2, _sp(yy, source, x), which).start()

    def w_rest(which):
        for yy in (0, 1):
            for s in range(1, Z):
                w_copy(2, _sp(yy, (z + s) % Z, 1 - x), which).wait_recv()

            @pl.when(jnp.logical_not((c == 1 - x) & (y == yy)))
            def _():
                w_given(yy, 1 - x, which)

    def spread_wo(d):
        wo_copy(3, d).start()
        wo_copy(4, d).start()

    def pass_wo(s):
        @pl.when(c == x)
        def _():
            for way in (0, 1):
                source, there, on = arriving(s, way)

                @pl.when(there)
                def _():
                    wo_copy(way, _sp(y, source, c)).wait_recv()

                    @pl.when(on)
                    def _():
                        wo_copy(way, _sp(y, source, c)).start()

                    wo_copy(2, _sp(y, source, c)).start()
                    spread_wo(_sp(y, source, c))

    def twin_wo(s):
        @pl.when(c != x)
        def _():
            for way in (0, 1):
                source, there, _ = arriving(s, way)

                @pl.when(there)
                def _():
                    wo_copy(2, _sp(y, source, c)).wait_recv()
                    spread_wo(_sp(y, source, c))

    give_w(1)

    step = min(256, t)

    def turn(i, _):
        slot, at = i // (t // step), (i % (t // step)) * step
        token = ((slot // 2) * Z + z) * 2 * t + (slot % 2) * t + at + lax.broadcasted_iota(jnp.int32, (step, HEAD // 2), 0)
        angle = token.astype(jnp.float32) * freq_ref[...]
        cos_s[pl.ds(i * step, step), :] = jnp.cos(angle)
        sin_s[pl.ds(i * step, step), :] = jnp.sin(angle)

    lax.fori_loop(0, 4 * t // step, turn, None)
    for s in range(1, Z):
        pass_w(s, 1)
    give_w(0)
    own_wo().wait()

    @pl.when(c == x)
    def _():
        for way in (0, 1):

            @pl.when(goes[way])
            def _():
                wo_copy(way, me).start()

    spread_wo(me)
    w_rest(1)

    half = HEAD // 2

    def turned(got, i, here):
        u, w = got[:, i * HEAD : i * HEAD + half], got[:, i * HEAD + half : (i + 1) * HEAD]
        cos, sin = cos_s[here, :], sin_s[here, :]
        return jnp.concatenate([u * cos - w * sin, w * cos + u * sin], -1).astype(jnp.bfloat16)

    def product(slot, at, columns):
        got = jnp.dot(a_s[slot, pl.ds(at, step), :], w_s[:, columns], preferred_element_type=jnp.float32)
        return got.astype(jnp.bfloat16).astype(jnp.float32)

    def keys_values(slot, at):
        got = product(slot, at, slice(2 * HEAD, 4 * HEAD))
        there = pl.ds(pl.multiple_of((slot % 2) * t + at, 128), step)
        k_s[z, slot // 2, there, :] = turned(got, 0, pl.ds(slot * t + at, step))
        v_s[z, slot // 2, :, there] = got[:, HEAD:].T.astype(jnp.bfloat16)

    def queries(slot, at):
        got = product(slot, at, slice(0, 2 * HEAD))
        for n in (0, 1):
            q_s[slot * 2 + n, pl.ds(at, step), :] = turned(got, n, pl.ds(slot * t + at, step))

    per = t // step

    def unit_copies(source, e, way):
        to = (x, _sp(y, jnp.clip(z + 1 - 2 * way, 0, Z - 1), c))
        k_at, v_at = k_s.at[source, e], v_s.at[source, e]
        return (
            _send(k_at, k_at, k_send.at[way, source, e], k_recv.at[source, e], to),
            _send(v_at, v_at, v_send.at[way, source, e], v_recv.at[source, e], to),
        )

    def give_unit(e):
        @pl.when(z < Z - 1 - e)
        def _():
            for copy in unit_copies(z, e, 0):
                copy.start()

        @pl.when((z > 0) & (e == 0))
        def _():
            for copy in unit_copies(z, e, 1):
                copy.start()

    for p in range(PIECES):
        a_copy(0, beside_slot, p).wait_recv()
    lax.fori_loop(0, 2 * per, lambda i, _: keys_values(2 * y + i // per, (i % per) * step), None)
    for s in range(1, Z):
        pass_w(s, 0)
    pass_wo(1)
    give_unit(y)
    w_rest(0)
    lax.fori_loop(0, 2 * per, lambda i, _: queries(2 * y + i // per, (i % per) * step), None)
    pass_wo(2)

    def others(i, _):
        for p in range(PIECES // per):
            relay_a(i * (PIECES // per) + p)
        keys_values(over, i * step)
        for p in range(PIECES // per):
            a_copy(2, diagonal_slot, i * (PIECES // per) + p).wait_recv()
        keys_values(diagonal_slot, i * step)

    lax.fori_loop(0, per, others, None)
    give_unit(1 - y)
    twin_wo(1)
    lax.fori_loop(0, 2 * per, lambda i, _: queries(2 * (1 - y) + i // per, (i % per) * step), None)

    def help_copy(i):
        if i == 0:
            return _send(q_s.at[4:8], q_s.at[8:12], help_send.at[0], help_recv.at[0], along[1])
        place = part_s if i == 1 else stat_s
        return _send(place, place, help_send.at[i], help_recv.at[i], along[1])

    @pl.when(helped)
    def _():
        help_copy(0).start()

    pass_wo(3)

    top_s[...] = jnp.full(top_s.shape, NEG, jnp.float32)
    mix_s[...] = jnp.zeros(mix_s.shape, jnp.float32)
    ones = jnp.ones((8, t), jnp.bfloat16)

    def block(source, e, j, strips, masked):
        here = pl.ds(pl.multiple_of(j * t, 128), t)
        keys = k_s[source, e, here, :]
        values = jnp.concatenate([v_s[source, e, :, here], ones], axis=0)
        scores = [_dot(keys, q_s[i], 1, 1) for i in strips]
        weights, keeps = [], []
        for i, s in zip(strips, scores):
            if masked:
                ok = lax.broadcasted_iota(jnp.int32, (t, t), 1) >= lax.broadcasted_iota(jnp.int32, (t, t), 0)
                s = jnp.where(ok, s, HIDDEN)
            old = top_s[i]
            top = jnp.maximum(old, s.max(axis=0, keepdims=True))
            top_s[i] = top
            weights.append(jnp.exp2((s - top) * e_scale).astype(jnp.bfloat16))
            keeps.append(jnp.exp2((old - top) * e_scale))
        for i, p, keep in zip(strips, weights, keeps):
            mix_s[i] = mix_s[i] * keep + _dot(values, p, 1, 0)

    def full(source, e, g, j):
        block(source, e, j, [4 * g + i for i in range(4)], False)

    def diagonal(i, _):
        g, j = i // 2, i % 2
        block(z, g, j, [4 * g + 2 * j, 4 * g + 2 * j + 1], True)

    lax.fori_loop(0, 4, diagonal, None)
    lax.fori_loop(0, 2, lambda g, _: block(z, g, 0, [4 * g + 2, 4 * g + 3], False), None)

    def result(to):
        return _send(o_s.at[to], og_s.at[h], o_send.at[to], o_recv.at[h], (x, _sp(to // 2, z, to % 2)))

    def settle(i, s4, n):
        o_s[s4, :, n * HEAD : (n + 1) * HEAD] = (mix_s[i, :HEAD, :] * (1 / mix_s[i, HEAD : HEAD + 1, :])).T.astype(jnp.bfloat16)

    def finish(g):
        def slot(i, _):
            s4 = 2 * g + i
            for n in (0, 1):
                settle(2 * s4 + n, s4, n)

            @pl.when(s4 != h)
            def _():
                result(s4).start()

        lax.fori_loop(0, 2, slot, None)

    def give_part():
        for n in range(4):
            i = 4 + n
            total = mix_s[i, HEAD : HEAD + 1, :]
            part_s[n] = (mix_s[i, :HEAD, :] * (1 / total)).astype(jnp.bfloat16)
            stat_s[n, 0:1, :] = top_s[i]
            stat_s[n, 1:2, :] = total
        help_copy(1).start()
        help_copy(2).start()

    def helped_result(cc):
        return _send(help_s.at[cc], og_s.at[h], help_send.at[3 + cc], o_recv.at[h], taker[cc])

    def finish_help():
        help_copy(1).wait_recv()
        help_copy(2).wait_recv()
        for cc in (0, 1):
            for n in (0, 1):
                i, k = 8 + 2 * cc + n, 2 * cc + n
                old, new = top_s[i], stat_s[k, 0:1, :]
                top = jnp.maximum(old, new)
                keep, gain = jnp.exp2((old - top) * e_scale), jnp.exp2((new - top) * e_scale) * stat_s[k, 1:2, :]
                total = mix_s[i, HEAD : HEAD + 1, :] * keep + gain
                both = mix_s[i, :HEAD, :] * keep + part_s[k].astype(jnp.float32) * gain
                help_s[cc, :, n * HEAD : (n + 1) * HEAD] = (both * (1 / total)).T.astype(jnp.bfloat16)
            helped_result(cc).start()

    def unit(i, _):
        s, kind = (i + 2) // 3, (i + 2) % 3
        sign = jnp.where(kind == 1, -1, 1)
        source = z - sign * s
        e = jnp.where(s == 0, 0, kind // 2)
        there = (source >= 0) & (source < Z) & ((e == 0) | jnp.logical_not(helped))
        both = helps & (s == 2) & (kind != 1)

        @pl.when(there)
        def _():
            @pl.when(s > 0)
            def _():
                way = jnp.where(kind == 1, 1, 0)
                for copy in unit_copies(source, e, way):
                    copy.wait_recv()
                on = z + sign

                @pl.when((on >= 0) & (on < Z - e))
                def _():
                    for copy in unit_copies(source, e, way):
                        copy.start()

            most = jnp.where(both, 2, jnp.where(helped & (s > 0), 0, 1))
            least = jnp.where(kind == 0, 0, 1)

            def work(u, _):
                full(source, e, most - u // 2, u % 2)

                @pl.when(both & (kind == 2) & (u == 1))
                def _():
                    finish_help()

            lax.fori_loop(0, 2 * (most + 1 - least), work, None)

            @pl.when(((kind == 0) & (s == z)) | ((s == 0) & (z == 0)))
            def _():
                finish(0)

    lax.fori_loop(0, 1, unit, None)

    @pl.when(helped)
    def _():
        give_part()

    lax.fori_loop(1, 4, unit, None)
    twin_wo(2)
    twin_wo(3)

    @pl.when(helps)
    def _():
        help_copy(0).wait_recv()
        lax.fori_loop(0, 8, lambda u, _: full(z - u // 4, (u // 2) % 2, 2, u % 2), None)

    lax.fori_loop(4, 3 * Z - 2, unit, None)

    @pl.when(jnp.logical_not(helped))
    def _():
        finish(1)

    for zz in range(Z):
        wo_copy(3, _sp(1 - y, zz, c)).wait_recv()
        wo_copy(4, _sp(1 - y, zz, c)).start()

    for zz in range(Z):
        for yy in (0, 1):
            wo_copy(4, _sp(yy, zz, 1 - c)).wait_recv()

    @pl.when(served)
    def _():
        _send(og_s.at[h], og_s.at[h], o_send.at[h], o_recv.at[h], twin).wait_recv()

    @pl.when(jnp.logical_not(served))
    def _():
        og_s[h] = o_s[h]

    for j in (1, 2, 3):
        other = (h + j) % 4
        _send(og_s.at[other], og_s.at[other], o_send.at[other], o_recv.at[other], twin).wait_recv()
    wide = 256

    def output(i, _):
        at = pl.ds(pl.multiple_of(i * wide, 128), wide)
        total = x_ref[:, at].astype(jnp.float32)
        for n in range(4):
            total = total + jnp.dot(og_s[n], wo_s[n * 2 * HEAD : (n + 1) * 2 * HEAD, at], preferred_element_type=jnp.float32)
        y_ref[:, at] = total.astype(jnp.bfloat16)

    lax.fori_loop(0, x_ref.shape[1] // wide, output, None)

    for j in (1, 2, 3):
        for i in range(3):
            w_give(i, j).wait_send()

        @pl.when(((h + j) % 4 < 2) | jnp.logical_not(helped))
        def _():
            result((h + j) % 4).wait_send()

    for p in range(PIECES):
        a_copy(0, h, p).wait_send()
        a_copy(1, h, p).wait_send()
        a_copy(2, over, p).wait_send()
    for s in range(Z):
        for way in (0, 1):
            source, there, on = arriving(s, way)

            @pl.when(there & on)
            def _():
                for yy in (0, 1):
                    for which in (0, 1):
                        w_copy(way, _sp(yy, source, x), which).wait_send()

                @pl.when(c == x)
                def _():
                    wo_copy(way, _sp(y, source, c)).wait_send()

            if s:

                @pl.when(there)
                def _():
                    for yy in (0, 1):
                        for which in (0, 1):
                            w_copy(2, _sp(yy, source, x), which).wait_send()

                    @pl.when(c == x)
                    def _():
                        wo_copy(2, _sp(y, source, c)).wait_send()

    for zz in range(Z):
        wo_copy(3, _sp(y, zz, c)).wait_send()
        wo_copy(4, _sp(y, zz, c)).wait_send()
        wo_copy(4, _sp(1 - y, zz, c)).wait_send()
    @pl.when(helped)
    def _():
        for i in range(3):
            help_copy(i).wait_send()

    @pl.when(helps)
    def _():
        for cc in (0, 1):
            helped_result(cc).wait_send()

    for source in range(Z):
        for e in (0, 1):

            @pl.when((z < Z - 1 - e) & (source <= z))
            def _():
                for copy in unit_copies(source, e, 0):
                    copy.wait_send()

            if e == 0:

                @pl.when((z > 0) & (source >= z))
                def _():
                    for copy in unit_copies(source, e, 1):
                        copy.wait_send()


def solution(mesh):
    half = HEAD // 2
    freq = np.power(np.float32(THETA), -np.arange(half, dtype=np.float32) / np.float32(half)).astype(np.float32)[None]

    def step(x, gain, wq, wk, wv, wo):
        t, d = x.shape
        vmem, far = pl.BlockSpec(memory_space=pltpu.VMEM), pl.BlockSpec(memory_space=pl.ANY)
        low, dma = jnp.bfloat16, pltpu.SemaphoreType.DMA
        return pl.pallas_call(
            _kernel,
            out_shape=jax.ShapeDtypeStruct((t, d), low),
            in_specs=[vmem, vmem, far, far, far, far, vmem],
            out_specs=vmem,
            scratch_shapes=[
                pltpu.VMEM((4, t, d), low),
                pltpu.VMEM((d, 4 * HEAD), low),
                pltpu.VMEM((8 * HEAD, d), low),
                pltpu.VMEM((4 * t, half), jnp.float32),
                pltpu.VMEM((4 * t, half), jnp.float32),
                pltpu.VMEM((12, t, HEAD), low),
                pltpu.VMEM((Z, 2, 2 * t, HEAD), low),
                pltpu.VMEM((Z, 2, HEAD, 2 * t), low),
                pltpu.VMEM((12, 1, t), jnp.float32),
                pltpu.VMEM((12, HEAD + 8, t), jnp.float32),
                pltpu.VMEM((4, t, 2 * HEAD), low),
                pltpu.VMEM((4, t, 2 * HEAD), low),
                pltpu.VMEM((4, HEAD, t), low),
                pltpu.VMEM((4, 8, t), jnp.float32),
                pltpu.VMEM((2, t, 2 * HEAD), low),
                dma((4,)),
                dma((3, 4)),
                dma((3, 2, 16)),
                dma((3, 16)),
                dma((5, 16)),
                dma((16,)),
                dma((3, PIECES)),
                dma((4, PIECES)),
                dma((2, Z, 2)),
                dma((Z, 2)),
                dma((2, Z, 2)),
                dma((Z, 2)),
                dma((4,)),
                dma((4,)),
                dma((5,)),
                dma((3,)),
            ],
            compiler_params=pltpu.CompilerParams(collective_id=0, has_side_effects=True, vmem_limit_bytes=VMEM),
            cost_estimate=pl.CostEstimate(flops=2 * t * d * 6144 + 8 * t * 16 * t * 4 * HEAD, bytes_accessed=48 * 2**20, transcendentals=0),
        )(x, gain[None], wq, wk, wv, wo, jnp.asarray(freq))

    tokens, whole = P(("dp", "sp"), None), P("sp", None)
    return jax.shard_map(
        step,
        mesh=mesh,
        in_specs=(tokens, P(None), whole, whole, whole, whole),
        out_specs=tokens,
        check_vma=False,
    )
```

```python
import jax
import jax.numpy as jnp
import numpy as np
from jax import lax
from jax.experimental import pallas as pl
from jax.experimental.pallas import tpu as pltpu
from jax.sharding import PartitionSpec as P


NEG = -1e30
HIDDEN = 2 * NEG
LOG2E = 1.4426950408889634
VMEM = 67043328
HEAD = 256
THETA = 10000
Z = 4
PIECES = 4
WIDE = 512
PAIR = (0, 1)
MESH = pl.DeviceIdType.MESH


def _dot(a, b, ca, cb):
    return lax.dot_general(a, b, (((ca,), (cb,)), ((), ())), preferred_element_type=jnp.float32)


def _loop(first, last, body):
    lax.fori_loop(first, last, body, None)


def _sp(y, z, c):
    return (y * Z + z) * 2 + c


def _send(src, dst, send_sem, recv_sem, device):
    return pltpu.make_async_remote_copy(src_ref=src, dst_ref=dst, send_sem=send_sem, recv_sem=recv_sem, device_id=device, device_id_type=MESH)


def _meet(always, sometimes):
    barrier = pltpu.get_barrier_semaphore()
    count = len(always)
    for device in always:
        pl.semaphore_signal(barrier, inc=1, device_id=device, device_id_type=MESH)
    for there, device in sometimes:

        @pl.when(there)
        def _():
            pl.semaphore_signal(barrier, inc=1, device_id=device, device_id_type=MESH)

        count = count + there.astype(jnp.int32)
    pl.semaphore_wait(barrier, count)


def _kernel(x_ref, gain_ref, wq_ref, wk_ref, wv_ref, wo_ref, freq_ref, y_ref, a_s, w_s, wo_s, cos_s, sin_s, q_s, k_s, v_s, top_s, mix_s, o_s, og_s, part_s, stat_s, help_s,
            own_sem, w_first, w_send, w_recv, wo_send, wo_recv, a_send, a_recv, k_send, k_recv, v_send, v_recv, o_send, o_recv, help_send, help_recv):
    x = lax.axis_index("dp")
    me = lax.axis_index("sp")
    y, z, c = me // (2 * Z), (me // 2) % Z, me % 2
    h = 2 * y + c
    t, r, ro = x_ref.shape[0], wq_ref.shape[0], wo_ref.shape[0]
    part = t // PIECES
    e_scale = HEAD**-0.5 * LOG2E
    beside, across, corner, twin = (x, _sp(y, z, 1 - c)), (x, _sp(1 - y, z, c)), (x, _sp(1 - y, z, 1 - c)), (1 - x, me)
    along = [(x, _sp(y, jnp.minimum(z + 1, Z - 1), c)), (x, _sp(y, jnp.maximum(z - 1, 0), c))]
    goes = [z < Z - 1, z > 0]
    helps, helped = z == Z - 2, z == Z - 1
    taker, served = [(x, _sp(1, Z - 1, cc)) for cc in PAIR], helped & (y == 1)
    _meet([beside, across, corner, twin], list(zip(goes, along)) + [(helps, device) for device in taker]
          + [(served, (x, _sp(yy, Z - 2, cc))) for yy in PAIR for cc in PAIR])

    def w_rows(d):
        return pl.ds(pl.multiple_of(d * r, 16), r)

    column = [0, WIDE, 3 * HEAD, 4 * HEAD]
    given = [wq_ref, wk_ref, wv_ref]

    def w_part(i, head):
        wide = column[i + 1] - column[i]
        return given[i].at[:, pl.ds(pl.multiple_of(head * wide, 128), wide)]

    def w_place(i, d):
        return w_s.at[w_rows(d), column[i] : column[i + 1]]

    def w_give(i, j):
        to = (h + j) % 4
        return _send(w_part(i, to), w_place(i, me), w_first.at[i, j], w_recv.at[i, me], (x, _sp(to // 2, z, to % 2)))

    def w_given(yy, cc, which):
        d = _sp(yy, z, cc)
        for i in (1, 2) if which else (0,):
            _send(w_place(i, d), w_place(i, d), w_first.at[i, 0], w_recv.at[i, d], twin).wait_recv()

    def w_copy(kind, d, which):
        place = w_s.at[w_rows(d), WIDE * which : WIDE * (which + 1)]
        return _send(place, place, w_send.at[kind, which, d], w_recv.at[which, d], twin if kind == 2 else along[kind])

    def own_w(i):
        return pltpu.make_async_copy(w_part(i, h), w_place(i, me), own_sem.at[i])

    def wo_copy(kind, d):
        place = wo_s.at[pl.ds(pl.multiple_of(d * ro, 16), ro), :]
        return _send(place, place, wo_send.at[kind, d], wo_recv.at[d], [along[0], along[1], twin, across, beside][kind])

    def own_wo():
        return pltpu.make_async_copy(wo_ref, wo_s.at[pl.ds(pl.multiple_of(me * ro, 16), ro), :], own_sem.at[3])

    def piece(slot, p):
        return a_s.at[slot, pl.ds(p * part, part), :]

    def a_copy(kind, slot, p):
        return _send(piece(slot, p), piece(slot, p), a_send.at[kind, p], a_recv.at[slot, p], across if kind == 1 else beside)

    over, diagonal_slot, beside_slot = 2 * (1 - y) + c, 2 * (1 - y) + 1 - c, 2 * y + 1 - c

    def relay_a(p):
        a_copy(1, over, p).wait_recv()
        a_copy(2, over, p).start()

    for which in (1, 0):
        for j in (1, 2, 3):
            for i in (1, 2) if which else (0,):
                w_give(i, j).start()
    for i in (1, 2, 0):
        own_w(i).start()
    own_wo().start()
    for p in range(PIECES):
        at = pl.ds(p * part, part)
        wide = x_ref[at, :].astype(jnp.float32)
        scale = lax.rsqrt(jnp.mean(wide * wide, -1, keepdims=True) + 1e-6)
        a_s[h, at, :] = (wide * scale * gain_ref[...].astype(jnp.float32)).astype(jnp.bfloat16)
        a_copy(1, h, p).start()
        a_copy(0, h, p).start()
    for i in range(3):
        own_w(i).wait()

    def give_w(which):
        for yy in PAIR:

            @pl.when(jnp.logical_not((c == x) & (y == yy)))
            def _():
                w_given(yy, x, which)

            for way in PAIR:

                @pl.when(goes[way])
                def _():
                    w_copy(way, _sp(yy, z, x), which).start()

    def arriving(s, way):
        source = z - s if way == 0 else z + s
        return source, (source >= 0) & (source < Z), goes[way]

    def pass_w(s, which):
        for way in PAIR:
            source, there, on = arriving(s, way)

            @pl.when(there)
            def _():
                for yy in PAIR:
                    w_copy(way, _sp(yy, source, x), which).wait_recv()

                    @pl.when(on)
                    def _():
                        w_copy(way, _sp(yy, source, x), which).start()

                    w_copy(2, _sp(yy, source, x), which).start()

    def w_rest(which):
        for yy in PAIR:
            for s in range(1, Z):
                w_copy(2, _sp(yy, (z + s) % Z, 1 - x), which).wait_recv()

            @pl.when(jnp.logical_not((c == 1 - x) & (y == yy)))
            def _():
                w_given(yy, 1 - x, which)

    def spread_wo(d):
        wo_copy(3, d).start()
        wo_copy(4, d).start()

    def pass_wo(s):
        @pl.when(c == x)
        def _():
            for way in PAIR:
                source, there, on = arriving(s, way)

                @pl.when(there)
                def _():
                    wo_copy(way, _sp(y, source, c)).wait_recv()

                    @pl.when(on)
                    def _():
                        wo_copy(way, _sp(y, source, c)).start()

                    wo_copy(2, _sp(y, source, c)).start()
                    spread_wo(_sp(y, source, c))

    def twin_wo(s):
        @pl.when(c != x)
        def _():
            for way in PAIR:
                source, there, _ = arriving(s, way)

                @pl.when(there)
                def _():
                    wo_copy(2, _sp(y, source, c)).wait_recv()
                    spread_wo(_sp(y, source, c))

    give_w(1)

    step = min(256, t)

    def turn(i, _):
        slot, at = i // (t // step), (i % (t // step)) * step
        token = ((slot // 2) * Z + z) * 2 * t + (slot % 2) * t + at + lax.broadcasted_iota(jnp.int32, (step, HEAD // 2), 0)
        angle = token.astype(jnp.float32) * freq_ref[...]
        cos_s[pl.ds(i * step, step), :] = jnp.cos(angle)
        sin_s[pl.ds(i * step, step), :] = jnp.sin(angle)

    _loop(0, 4 * t // step, turn)
    for s in range(1, Z):
        pass_w(s, 1)
    give_w(0)
    own_wo().wait()

    @pl.when(c == x)
    def _():
        for way in PAIR:

            @pl.when(goes[way])
            def _():
                wo_copy(way, me).start()

    spread_wo(me)
    w_rest(1)

    half = HEAD // 2
    always = z >= 0

    def turned(got, i, here):
        u, w = got[:, i * HEAD : i * HEAD + half], got[:, i * HEAD + half : (i + 1) * HEAD]
        cos, sin = cos_s[here, :], sin_s[here, :]
        return jnp.concatenate([u * cos - w * sin, w * cos + u * sin], -1).astype(jnp.bfloat16)

    def product(slot, at, columns):
        got = jnp.dot(a_s[slot, pl.ds(at, step), :], w_s[:, columns], preferred_element_type=jnp.float32)
        return got.astype(jnp.bfloat16).astype(jnp.float32)

    def keys_values(slot, at):
        got = product(slot, at, slice(WIDE, 4 * HEAD))
        there = pl.ds(pl.multiple_of(at, 128), step)
        k_s[z, slot // 2, slot % 2, there, :] = turned(got, 0, pl.ds(slot * t + at, step))
        v_s[z, slot // 2, slot % 2, :, there] = got[:, HEAD:].T.astype(jnp.bfloat16)

    def queries(slot, at):
        got = product(slot, at, slice(0, WIDE))
        for n in PAIR:
            q_s[slot * 2 + n, pl.ds(at, step), :] = turned(got, n, pl.ds(slot * t + at, step))

    per = t // step

    def unit_copies(source, e, j, way):
        k_at, v_at = k_s.at[source, e, j], v_s.at[source, e, j]
        return (
            _send(k_at, k_at, k_send.at[way, source, e, j], k_recv.at[source, e, j], along[way]),
            _send(v_at, v_at, v_send.at[way, source, e, j], v_recv.at[source, e, j], along[way]),
        )

    def pass_unit(source, e, j, way, when):
        @pl.when(when & (z < Z - 1 - e if way == 0 else z > 0))
        def _():
            for copy in unit_copies(source, e, j, way):
                copy.start()

    def give_unit(e):
        for j in PAIR:
            pass_unit(z, e, j, 0, always)
            pass_unit(z, e, j, 1, e == 0)

    for p in range(PIECES):
        a_copy(0, beside_slot, p).wait_recv()
    _loop(0, 2 * per, lambda i, _: keys_values(2 * y + i // per, (i % per) * step))
    for s in range(1, Z):
        pass_w(s, 0)
    pass_wo(1)
    give_unit(y)
    w_rest(0)
    _loop(0, 2 * per, lambda i, _: queries(2 * y + i // per, (i % per) * step))
    pass_wo(2)

    def others(i, _):
        for p in range(PIECES // per):
            relay_a(i * (PIECES // per) + p)
        keys_values(over, i * step)
        for p in range(PIECES // per):
            a_copy(2, diagonal_slot, i * (PIECES // per) + p).wait_recv()
        keys_values(diagonal_slot, i * step)

    _loop(0, per, others)
    give_unit(1 - y)

    def relay_half(s, e, j, way, when):
        source = z - s if way == 0 else z + s

        @pl.when(when & (source >= 0) & (source < Z))
        def _():
            for copy in unit_copies(source, e, j, way):
                copy.wait_recv()
            pass_unit(source, e, j, way, always)

    def relay(s, e, way, when):
        for j in PAIR:
            relay_half(s, e, j, way, when)

    first, second = y == 0, y == 1
    relay(1, 0, 0, first)
    relay(1, 0, 1, first)
    twin_wo(1)
    _loop(0, 2 * per, lambda i, _: queries(2 * (1 - y) + i // per, (i % per) * step))

    def help_copy(i):
        if i == 0:
            return _send(q_s.at[4:8], q_s.at[8:12], help_send.at[0], help_recv.at[0], along[1])
        place = part_s if i == 1 else stat_s
        return _send(place, place, help_send.at[i], help_recv.at[i], along[1])

    @pl.when(helped)
    def _():
        help_copy(0).start()

    pass_wo(3)

    top_s[...] = jnp.full(top_s.shape, NEG, jnp.float32)
    mix_s[...] = jnp.zeros(mix_s.shape, jnp.float32)
    ones = jnp.ones((8, t), jnp.bfloat16)

    def block(source, e, j, strips, masked):
        keys = k_s[source, e, j]
        values = jnp.concatenate([v_s[source, e, j], ones], axis=0)
        scores = [_dot(keys, q_s[i], 1, 1) for i in strips]
        weights, keeps = [], []
        for i, s in zip(strips, scores):
            if masked:
                ok = lax.broadcasted_iota(jnp.int32, (t, t), 1) >= lax.broadcasted_iota(jnp.int32, (t, t), 0)
                s = jnp.where(ok, s, HIDDEN)
            old = top_s[i]
            top = jnp.maximum(old, s.max(axis=0, keepdims=True))
            top_s[i] = top
            weights.append(jnp.exp2((s - top) * e_scale).astype(jnp.bfloat16))
            keeps.append(jnp.exp2((old - top) * e_scale))
        for i, p, keep in zip(strips, weights, keeps):
            mix_s[i] = mix_s[i] * keep + _dot(values, p, 1, 0)

    def full(source, e, g, j):
        block(source, e, j, [4 * g + i for i in range(4)], False)

    def diagonal(i, _):
        g, j = i // 2, i % 2
        block(z, g, j, [4 * g + 2 * j, 4 * g + 2 * j + 1], True)

    _loop(0, 4, diagonal)
    _loop(0, 2, lambda g, _: block(z, g, 0, [4 * g + 2, 4 * g + 3], False))

    def result(to):
        return _send(o_s.at[to], og_s.at[h], o_send.at[to], o_recv.at[h], (x, _sp(to // 2, z, to % 2)))

    def settle(i, s4, n):
        o_s[s4, :, n * HEAD : (n + 1) * HEAD] = (mix_s[i, :HEAD, :] * (1 / mix_s[i, HEAD : HEAD + 1, :])).astype(jnp.bfloat16).T

    def finish(g):
        def slot(i, _):
            s4 = 2 * g + i
            for n in PAIR:
                settle(2 * s4 + n, s4, n)

            @pl.when(s4 != h)
            def _():
                result(s4).start()

        _loop(0, 2, slot)

    def give_part():
        for n in range(4):
            i = 4 + n
            total = mix_s[i, HEAD : HEAD + 1, :]
            part_s[n] = (mix_s[i, :HEAD, :] * (1 / total)).astype(jnp.bfloat16)
            stat_s[n, 0:1, :] = top_s[i]
            stat_s[n, 1:2, :] = total
        help_copy(1).start()
        help_copy(2).start()

    def helped_result(cc):
        return _send(help_s.at[cc], og_s.at[h], help_send.at[3 + cc], o_recv.at[h], taker[cc])

    def finish_help():
        help_copy(1).wait_recv()
        help_copy(2).wait_recv()
        for cc in PAIR:
            for n in PAIR:
                i, k = 8 + 2 * cc + n, 2 * cc + n
                old, new = top_s[i], stat_s[k, 0:1, :]
                top = jnp.maximum(old, new)
                keep, gain = jnp.exp2((old - top) * e_scale), jnp.exp2((new - top) * e_scale) * stat_s[k, 1:2, :]
                total = mix_s[i, HEAD : HEAD + 1, :] * keep + gain
                both = mix_s[i, :HEAD, :] * keep + part_s[k].astype(jnp.float32) * gain
                help_s[cc, :, n * HEAD : (n + 1) * HEAD] = (both * (1 / total)).astype(jnp.bfloat16).T
            helped_result(cc).start()

    def stage(entries, halves=PAIR, then=None):
        per_strip = len(halves)

        def entry(k, _):
            def pick(n):
                got = jnp.asarray(entries[0][n])
                for i in range(1, len(entries)):
                    got = jnp.where(k == i, entries[i][n], got)
                return got

            source, e, least, most, go = (pick(n) for n in range(5))

            def work(u, _):
                full(source, e, most - u // per_strip, halves[0] + u % per_strip)
                if then is not None:

                    @pl.when(u == 0)
                    def _():
                        then()

            _loop(0, jnp.where(go, per_strip * (most + 1 - least), 0), work)

        _loop(0, len(entries), entry)

    mine = jnp.where(helped, 0, 1)
    stage([(z, 0, 1, 1, always), (z - 1, 0, 0, mine, first & (z > 0)), (z + 1, 0, 1, 1, first & (z < Z - 1))])

    @pl.when(helped)
    def _():
        give_part()

    @pl.when(z == 0)
    def _():
        finish(0)

    twin_wo(2)
    twin_wo(3)
    relay(1, 0, 0, second)
    relay(1, 0, 1, second)
    relay(2, 0, 1, first)
    relay(1, 1, 0, jnp.logical_not(helped))
    stage([(z - 1, 0, 0, mine, second & (z > 0)), (z + 2 - y, 0, 1, 1, z + 2 - y < Z), (z - 1, 1, 1, 1, (z > 0) & jnp.logical_not(helped))])

    @pl.when(z == 1)
    def _():
        finish(0)

    relay(2, 0, 0, always)
    relay(3, 0, 1, first)
    relay(2, 0, 1, second)

    @pl.when(helps)
    def _():
        help_copy(0).wait_recv()

    stage([(z - 2, 0, 0, jnp.where(helps, 2, mine), z >= 2), (z + 3 - y, 0, 1, 1, z + 3 - y < Z)]
          + [(z - n // 2, n % 2, 2, 2, helps) for n in range(4)])

    @pl.when(helps)
    def _():
        finish(0)

    for zz in range(Z):
        wo_copy(3, _sp(1 - y, zz, c)).wait_recv()
        wo_copy(4, _sp(1 - y, zz, c)).start()

    def helper_done():
        @pl.when(helps)
        def _():
            finish_help()

    last_unit = (jnp.where(helps, z - 2, jnp.where(helped, z - 3, z + 3)), jnp.where(helps, 1, 0), jnp.where(helped, 0, 1),
                 jnp.where(helps, 2, mine), helps | helped | (second & (z == 0)))
    for j in PAIR:
        relay_half(2, 1, j, 0, helps)
        relay_half(3, 0, j, 0, always)
        relay_half(3, 0, j, 1, second)
        stage([last_unit], (j,), helper_done if j else None)

    @pl.when(helped)
    def _():
        finish(0)

    @pl.when(jnp.logical_not(helped))
    def _():
        finish(1)

    for zz in range(Z):
        for yy in PAIR:
            wo_copy(4, _sp(yy, zz, 1 - c)).wait_recv()

    def result_wait(head):
        _send(og_s.at[head], og_s.at[head], o_send.at[head], o_recv.at[head], twin).wait_recv()

    @pl.when(served)
    def _():
        result_wait(h)

    @pl.when(jnp.logical_not(served))
    def _():
        og_s[h] = o_s[h]

    result_wait(beside_slot)
    low_rows = t // 2

    def output(n, two, final):
        at = pl.ds(pl.multiple_of(n * low_rows, 128), low_rows)
        if final:
            total = jnp.concatenate([mix_s[n, :low_rows, :low_rows], mix_s[n, :low_rows, low_rows:]], axis=0)
        else:
            total = x_ref[:, at].astype(jnp.float32)
        for head in two:
            there = pl.ds(pl.multiple_of(head * WIDE, WIDE), WIDE)
            total = total + jnp.dot(og_s[head], wo_s[there, at], preferred_element_type=jnp.float32)
        if final:
            y_ref[:, at] = total.astype(jnp.bfloat16)
        else:
            mix_s[n, :low_rows, :low_rows] = total[:low_rows]
            mix_s[n, :low_rows, low_rows:] = total[low_rows:]

    tiles = x_ref.shape[1] // low_rows
    _loop(0, tiles, lambda n, _: output(n, (h, beside_slot), False))
    result_wait(over)
    result_wait(diagonal_slot)
    _loop(0, tiles, lambda n, _: output(n, (over, diagonal_slot), True))

    for j in (1, 2, 3):
        for i in range(3):
            w_give(i, j).wait_send()

        @pl.when(((h + j) % 4 < 2) | jnp.logical_not(helped))
        def _():
            result((h + j) % 4).wait_send()

    for p in range(PIECES):
        a_copy(0, h, p).wait_send()
        a_copy(1, h, p).wait_send()
        a_copy(2, over, p).wait_send()
    for s in range(Z):
        for way in PAIR:
            source, there, on = arriving(s, way)

            @pl.when(there & on)
            def _():
                for yy in PAIR:
                    for which in PAIR:
                        w_copy(way, _sp(yy, source, x), which).wait_send()

                @pl.when(c == x)
                def _():
                    wo_copy(way, _sp(y, source, c)).wait_send()

            if s:

                @pl.when(there)
                def _():
                    for yy in PAIR:
                        for which in PAIR:
                            w_copy(2, _sp(yy, source, x), which).wait_send()

                    @pl.when(c == x)
                    def _():
                        wo_copy(2, _sp(y, source, c)).wait_send()

    for zz in range(Z):
        wo_copy(3, _sp(y, zz, c)).wait_send()
        wo_copy(4, _sp(y, zz, c)).wait_send()
        wo_copy(4, _sp(1 - y, zz, c)).wait_send()
    @pl.when(helped)
    def _():
        for i in range(3):
            help_copy(i).wait_send()

    @pl.when(helps)
    def _():
        for cc in PAIR:
            helped_result(cc).wait_send()

    for source in range(Z):
        for e in PAIR:
            for way in PAIR[: 2 - e]:

                @pl.when((z < Z - 1 - e) & (source <= z) if way == 0 else (z > 0) & (source >= z))
                def _():
                    for j in PAIR:
                        for copy in unit_copies(source, e, j, way):
                            copy.wait_send()


def solution(mesh):
    half = HEAD // 2
    freq = np.power(np.float32(THETA), -np.arange(half, dtype=np.float32) / np.float32(half)).astype(np.float32)[None]

    def step(x, gain, wq, wk, wv, wo):
        t, d = x.shape
        vmem, far = pl.BlockSpec(memory_space=pltpu.VMEM), pl.BlockSpec(memory_space=pl.ANY)
        low, dma = jnp.bfloat16, pltpu.SemaphoreType.DMA
        return pl.pallas_call(
            _kernel,
            out_shape=jax.ShapeDtypeStruct((t, d), low),
            in_specs=[vmem, vmem, far, far, far, far, vmem],
            out_specs=vmem,
            scratch_shapes=[
                pltpu.VMEM((4, t, d), low),
                pltpu.VMEM((d, 4 * HEAD), low),
                pltpu.VMEM((8 * HEAD, d), low),
                pltpu.VMEM((4 * t, half), jnp.float32),
                pltpu.VMEM((4 * t, half), jnp.float32),
                pltpu.VMEM((12, t, HEAD), low),
                pltpu.VMEM((Z, 2, 2, t, HEAD), low),
                pltpu.VMEM((Z, 2, 2, HEAD, t), low),
                pltpu.VMEM((12, 1, t), jnp.float32),
                pltpu.VMEM((12, HEAD + 8, t), jnp.float32),
                pltpu.VMEM((4, t, WIDE), low),
                pltpu.VMEM((4, t, WIDE), low),
                pltpu.VMEM((4, HEAD, t), low),
                pltpu.VMEM((4, 8, t), jnp.float32),
                pltpu.VMEM((2, t, WIDE), low),
                dma((4,)),
                dma((3, 4)),
                dma((3, 2, 16)),
                dma((3, 16)),
                dma((5, 16)),
                dma((16,)),
                dma((3, PIECES)),
                dma((4, PIECES)),
                dma((2, Z, 2, 2)),
                dma((Z, 2, 2)),
                dma((2, Z, 2, 2)),
                dma((Z, 2, 2)),
                dma((4,)),
                dma((4,)),
                dma((5,)),
                dma((3,)),
            ],
            compiler_params=pltpu.CompilerParams(collective_id=0, has_side_effects=True, vmem_limit_bytes=VMEM),
            cost_estimate=pl.CostEstimate(flops=2 * t * d * 6144 + 8 * t * 16 * t * 4 * HEAD, bytes_accessed=48 * 2**20, transcendentals=0),
        )(x, gain[None], wq, wk, wv, wo, jnp.asarray(freq))

    tokens, whole = P(("dp", "sp"), None), P("sp", None)
    return jax.shard_map(
        step,
        mesh=mesh,
        in_specs=(tokens, P(None), whole, whole, whole, whole),
        out_specs=tokens,
        check_vma=False,
    )
```

```python
import jax
import jax.numpy as jnp
import numpy as np
from jax import lax
from jax.experimental import pallas as pl
from jax.experimental.pallas import tpu as pltpu
from jax.sharding import PartitionSpec as P


NEG = -1e30
HIDDEN = 2 * NEG
LOG2E = 1.4426950408889634
VMEM = 67043328
HEAD = 256
THETA = 10000
Z = 4
PIECES = 4
WIDE = 512
PAIR = (0, 1)
MESH = pl.DeviceIdType.MESH


def _dot(a, b, ca, cb):
    return lax.dot_general(a, b, (((ca,), (cb,)), ((), ())), preferred_element_type=jnp.float32)


def _loop(first, last, body):
    lax.fori_loop(first, last, body, None)


def _sp(y, z, c):
    return (y * Z + z) * 2 + c


def _send(src, dst, send_sem, recv_sem, device):
    return pltpu.make_async_remote_copy(src_ref=src, dst_ref=dst, send_sem=send_sem, recv_sem=recv_sem, device_id=device, device_id_type=MESH)


def _meet(always, sometimes):
    barrier = pltpu.get_barrier_semaphore()
    count = len(always)
    for device in always:
        pl.semaphore_signal(barrier, inc=1, device_id=device, device_id_type=MESH)
    for there, device in sometimes:

        @pl.when(there)
        def _():
            pl.semaphore_signal(barrier, inc=1, device_id=device, device_id_type=MESH)

        count = count + there.astype(jnp.int32)
    pl.semaphore_wait(barrier, count)


def _kernel(x_ref, gain_ref, wq_ref, wk_ref, wv_ref, wo_ref, freq_ref, y_ref, a_s, w_s, wo_s, cos_s, sin_s, q_s, k_s, v_s, top_s, mix_s, o_s, og_s, part_s, stat_s, help_s,
            own_sem, w_first, w_send, w_recv, wo_send, wo_recv, a_send, a_recv, k_send, k_recv, v_send, v_recv, o_send, o_recv, help_send, help_recv):
    x = lax.axis_index("dp")
    me = lax.axis_index("sp")
    y, z, c = me // (2 * Z), (me // 2) % Z, me % 2
    h = 2 * y + c
    t, r, ro = x_ref.shape[0], wq_ref.shape[0], wo_ref.shape[0]
    part = t // PIECES
    e_scale = HEAD**-0.5 * LOG2E
    beside, across, corner, twin = (x, _sp(y, z, 1 - c)), (x, _sp(1 - y, z, c)), (x, _sp(1 - y, z, 1 - c)), (1 - x, me)
    along = [(x, _sp(y, jnp.minimum(z + 1, Z - 1), c)), (x, _sp(y, jnp.maximum(z - 1, 0), c))]
    goes = [z < Z - 1, z > 0]
    helps, helped = z == Z - 2, z == Z - 1
    taker, served = [(x, _sp(1, Z - 1, cc)) for cc in PAIR], helped & (y == 1)
    _meet([beside, across, corner, twin], list(zip(goes, along)) + [(helps, device) for device in taker]
          + [(served, (x, _sp(yy, Z - 2, cc))) for yy in PAIR for cc in PAIR])

    def w_rows(d):
        return pl.ds(pl.multiple_of(d * r, 16), r)

    column = [0, WIDE, 3 * HEAD, 4 * HEAD]
    given = [wq_ref, wk_ref, wv_ref]

    def w_part(i, head):
        wide = column[i + 1] - column[i]
        return given[i].at[:, pl.ds(pl.multiple_of(head * wide, 128), wide)]

    def w_place(i, d):
        return w_s.at[w_rows(d), column[i] : column[i + 1]]

    def w_give(i, j):
        to = (h + j) % 4
        return _send(w_part(i, to), w_place(i, me), w_first.at[i, j], w_recv.at[i, me], (x, _sp(to // 2, z, to % 2)))

    def w_given(yy, cc, which):
        d = _sp(yy, z, cc)
        for i in (1, 2) if which else (0,):
            _send(w_place(i, d), w_place(i, d), w_first.at[i, 0], w_recv.at[i, d], twin).wait_recv()

    def w_copy(kind, d, which):
        place = w_s.at[w_rows(d), WIDE * which : WIDE * (which + 1)]
        return _send(place, place, w_send.at[kind, which, d], w_recv.at[which, d], twin if kind == 2 else along[kind])

    def own_w(i):
        return pltpu.make_async_copy(w_part(i, h), w_place(i, me), own_sem.at[i])

    def wo_copy(kind, d):
        place = wo_s.at[pl.ds(pl.multiple_of(d * ro, 16), ro), :]
        return _send(place, place, wo_send.at[kind, d], wo_recv.at[d], [along[0], along[1], twin, across, beside][kind])

    def own_wo():
        return pltpu.make_async_copy(wo_ref, wo_s.at[pl.ds(pl.multiple_of(me * ro, 16), ro), :], own_sem.at[3])

    def piece(slot, p):
        return a_s.at[slot, pl.ds(p * part, part), :]

    def a_copy(kind, slot, p):
        return _send(piece(slot, p), piece(slot, p), a_send.at[kind, p], a_recv.at[slot, p], across if kind == 1 else beside)

    over, diagonal_slot, beside_slot = 2 * (1 - y) + c, 2 * (1 - y) + 1 - c, 2 * y + 1 - c

    def relay_a(p):
        a_copy(1, over, p).wait_recv()
        a_copy(2, over, p).start()

    for which in (1, 0):
        for j in (1, 2, 3):

            @pl.when((c == x) | ((h + j) % 4 // 2 == y))
            def _():
                for i in (1, 2) if which else (0,):
                    w_give(i, j).start()

    for i in (1, 2, 0):
        own_w(i).start()
    own_wo().start()
    for p in range(PIECES):
        at = pl.ds(p * part, part)
        wide = x_ref[at, :].astype(jnp.float32)
        scale = lax.rsqrt(jnp.mean(wide * wide, -1, keepdims=True) + 1e-6)
        a_s[h, at, :] = (wide * scale * gain_ref[...].astype(jnp.float32)).astype(jnp.bfloat16)
        a_copy(1, h, p).start()
        a_copy(0, h, p).start()
    for i in range(3):
        own_w(i).wait()

    def give_w(which):
        for yy in PAIR:

            @pl.when(jnp.logical_not((c == x) & (y == yy)))
            def _():
                w_given(yy, x, which)

            @pl.when(y != yy)
            def _():
                w_copy(2, _sp(yy, z, x), which).start()

            for way in PAIR:

                @pl.when(goes[way])
                def _():
                    w_copy(way, _sp(yy, z, x), which).start()

    def arriving(s, way):
        source = z - s if way == 0 else z + s
        return source, (source >= 0) & (source < Z), goes[way]

    def pass_w(s, which):
        for way in PAIR:
            source, there, on = arriving(s, way)

            @pl.when(there)
            def _():
                for yy in PAIR:
                    w_copy(way, _sp(yy, source, x), which).wait_recv()

                    @pl.when(on)
                    def _():
                        w_copy(way, _sp(yy, source, x), which).start()

                    w_copy(2, _sp(yy, source, x), which).start()

    def w_rest(which):
        for yy in PAIR:
            for s in range(1, Z):
                w_copy(2, _sp(yy, (z + s) % Z, 1 - x), which).wait_recv()
        w_copy(2, _sp(1 - y, z, 1 - x), which).wait_recv()

        @pl.when(c == x)
        def _():
            w_given(y, 1 - x, which)

    def spread_wo(d):
        wo_copy(3, d).start()
        wo_copy(4, d).start()

    def pass_wo(s):
        @pl.when(c == x)
        def _():
            for way in PAIR:
                source, there, on = arriving(s, way)

                @pl.when(there)
                def _():
                    wo_copy(way, _sp(y, source, c)).wait_recv()

                    @pl.when(on)
                    def _():
                        wo_copy(way, _sp(y, source, c)).start()

                    wo_copy(2, _sp(y, source, c)).start()
                    spread_wo(_sp(y, source, c))

    def twin_wo(s):
        @pl.when(c != x)
        def _():
            for way in PAIR:
                source, there, _ = arriving(s, way)

                @pl.when(there)
                def _():
                    wo_copy(2, _sp(y, source, c)).wait_recv()
                    spread_wo(_sp(y, source, c))

    give_w(1)

    step = min(256, t)

    def turn(i, _):
        slot, at = i // (t // step), (i % (t // step)) * step
        token = ((slot // 2) * Z + z) * 2 * t + (slot % 2) * t + at + lax.broadcasted_iota(jnp.int32, (step, HEAD // 2), 0)
        angle = token.astype(jnp.float32) * freq_ref[...]
        cos_s[pl.ds(i * step, step), :] = jnp.cos(angle)
        sin_s[pl.ds(i * step, step), :] = jnp.sin(angle)

    _loop(0, 4 * t // step, turn)
    for s in range(1, Z):
        pass_w(s, 1)
    give_w(0)
    own_wo().wait()

    @pl.when(c == x)
    def _():
        for way in PAIR:

            @pl.when(goes[way])
            def _():
                wo_copy(way, me).start()

    spread_wo(me)
    w_rest(1)

    half = HEAD // 2
    always = z >= 0

    def turned(got, i, here):
        u, w = got[:, i * HEAD : i * HEAD + half], got[:, i * HEAD + half : (i + 1) * HEAD]
        cos, sin = cos_s[here, :], sin_s[here, :]
        return jnp.concatenate([u * cos - w * sin, w * cos + u * sin], -1).astype(jnp.bfloat16)

    def product(slot, at, columns):
        got = jnp.dot(a_s[slot, pl.ds(at, step), :], w_s[:, columns], preferred_element_type=jnp.float32)
        return got.astype(jnp.bfloat16).astype(jnp.float32)

    def keys_values(slot, at):
        got = product(slot, at, slice(WIDE, 4 * HEAD))
        there = pl.ds(pl.multiple_of(at, 128), step)
        k_s[z, slot // 2, slot % 2, there, :] = turned(got, 0, pl.ds(slot * t + at, step))
        v_s[z, slot // 2, slot % 2, :, there] = got[:, HEAD:].T.astype(jnp.bfloat16)

    def queries(slot, at):
        got = product(slot, at, slice(0, WIDE))
        for n in PAIR:
            q_s[slot * 2 + n, pl.ds(at, step), :] = turned(got, n, pl.ds(slot * t + at, step))

    per = t // step

    def unit_copies(source, e, j, way):
        k_at, v_at = k_s.at[source, e, j], v_s.at[source, e, j]
        return (
            _send(k_at, k_at, k_send.at[way, source, e, j], k_recv.at[source, e, j], along[way]),
            _send(v_at, v_at, v_send.at[way, source, e, j], v_recv.at[source, e, j], along[way]),
        )

    def pass_unit(source, e, j, way, when):
        @pl.when(when & (z < Z - 1 - e if way == 0 else z > 0))
        def _():
            for copy in unit_copies(source, e, j, way):
                copy.start()

    def give_unit(e):
        for j in PAIR:
            pass_unit(z, e, j, 0, always)
            pass_unit(z, e, j, 1, e == 0)

    for p in range(PIECES):
        a_copy(0, beside_slot, p).wait_recv()
    _loop(0, 2 * per, lambda i, _: keys_values(2 * y + i // per, (i % per) * step))
    for s in range(1, Z):
        pass_w(s, 0)
    pass_wo(1)
    give_unit(y)
    w_rest(0)
    _loop(0, 2 * per, lambda i, _: queries(2 * y + i // per, (i % per) * step))
    pass_wo(2)

    def others(i, _):
        for p in range(PIECES // per):
            relay_a(i * (PIECES // per) + p)
        keys_values(over, i * step)
        for p in range(PIECES // per):
            a_copy(2, diagonal_slot, i * (PIECES // per) + p).wait_recv()
        keys_values(diagonal_slot, i * step)

    _loop(0, per, others)
    give_unit(1 - y)

    def relay_half(s, e, j, way, when):
        source = z - s if way == 0 else z + s

        @pl.when(when & (source >= 0) & (source < Z))
        def _():
            for copy in unit_copies(source, e, j, way):
                copy.wait_recv()
            pass_unit(source, e, j, way, always)

    def relay(s, e, way, when):
        for j in PAIR:
            relay_half(s, e, j, way, when)

    first, second = y == 0, y == 1
    relay(1, 0, 0, first)
    relay(1, 0, 1, first)
    twin_wo(1)
    _loop(0, 2 * per, lambda i, _: queries(2 * (1 - y) + i // per, (i % per) * step))

    def help_copy(i):
        if i == 0:
            return _send(q_s.at[4:8], q_s.at[8:12], help_send.at[0], help_recv.at[0], along[1])
        place = part_s if i == 1 else stat_s
        return _send(place, place, help_send.at[i], help_recv.at[i], along[1])

    @pl.when(helped)
    def _():
        help_copy(0).start()

    pass_wo(3)

    top_s[...] = jnp.full(top_s.shape, NEG, jnp.float32)
    mix_s[...] = jnp.zeros(mix_s.shape, jnp.float32)
    ones = jnp.ones((8, t), jnp.bfloat16)

    def block(source, e, j, strips, masked):
        keys = k_s[source, e, j]
        values = jnp.concatenate([v_s[source, e, j], ones], axis=0)
        scores = [_dot(keys, q_s[i], 1, 1) for i in strips]
        weights, keeps = [], []
        for i, s in zip(strips, scores):
            if masked:
                ok = lax.broadcasted_iota(jnp.int32, (t, t), 1) >= lax.broadcasted_iota(jnp.int32, (t, t), 0)
                s = jnp.where(ok, s, HIDDEN)
            old = top_s[i]
            top = jnp.maximum(old, s.max(axis=0, keepdims=True))
            top_s[i] = top
            weights.append(jnp.exp2((s - top) * e_scale).astype(jnp.bfloat16))
            keeps.append(jnp.exp2((old - top) * e_scale))
        for i, p, keep in zip(strips, weights, keeps):
            mix_s[i] = mix_s[i] * keep + _dot(values, p, 1, 0)

    def full(source, e, g, j):
        block(source, e, j, [4 * g + i for i in range(4)], False)

    def diagonal(i, _):
        g, j = i // 2, i % 2
        block(z, g, j, [4 * g + 2 * j, 4 * g + 2 * j + 1], True)

    _loop(0, 4, diagonal)
    _loop(0, 2, lambda g, _: block(z, g, 0, [4 * g + 2, 4 * g + 3], False))

    def result(to):
        return _send(o_s.at[to], og_s.at[h], o_send.at[to], o_recv.at[h], (x, _sp(to // 2, z, to % 2)))

    def settle(i, s4, n):
        o_s[s4, :, n * HEAD : (n + 1) * HEAD] = (mix_s[i, :HEAD, :] * (1 / mix_s[i, HEAD : HEAD + 1, :])).astype(jnp.bfloat16).T

    def finish(g):
        def slot(i, _):
            s4 = 2 * g + i
            for n in PAIR:
                settle(2 * s4 + n, s4, n)

            @pl.when(s4 != h)
            def _():
                result(s4).start()

        _loop(0, 2, slot)

    def give_part():
        for n in range(4):
            i = 4 + n
            total = mix_s[i, HEAD : HEAD + 1, :]
            part_s[n] = (mix_s[i, :HEAD, :] * (1 / total)).astype(jnp.bfloat16)
            stat_s[n, 0:1, :] = top_s[i]
            stat_s[n, 1:2, :] = total
        help_copy(1).start()
        help_copy(2).start()

    def helped_result(cc):
        return _send(help_s.at[cc], og_s.at[h], help_send.at[3 + cc], o_recv.at[h], taker[cc])

    def finish_help():
        help_copy(1).wait_recv()
        help_copy(2).wait_recv()
        for cc in PAIR:
            for n in PAIR:
                i, k = 8 + 2 * cc + n, 2 * cc + n
                old, new = top_s[i], stat_s[k, 0:1, :]
                top = jnp.maximum(old, new)
                keep, gain = jnp.exp2((old - top) * e_scale), jnp.exp2((new - top) * e_scale) * stat_s[k, 1:2, :]
                total = mix_s[i, HEAD : HEAD + 1, :] * keep + gain
                both = mix_s[i, :HEAD, :] * keep + part_s[k].astype(jnp.float32) * gain
                help_s[cc, :, n * HEAD : (n + 1) * HEAD] = (both * (1 / total)).astype(jnp.bfloat16).T
            helped_result(cc).start()

    def stage(entries, halves=PAIR, then=None):
        per_strip = len(halves)

        def entry(k, _):
            def pick(n):
                got = jnp.asarray(entries[0][n])
                for i in range(1, len(entries)):
                    got = jnp.where(k == i, entries[i][n], got)
                return got

            source, e, least, most, go = (pick(n) for n in range(5))

            def work(u, _):
                full(source, e, most - u // per_strip, halves[0] + u % per_strip)
                if then is not None:

                    @pl.when(u == 0)
                    def _():
                        then()

            _loop(0, jnp.where(go, per_strip * (most + 1 - least), 0), work)

        _loop(0, len(entries), entry)

    mine = jnp.where(helped, 0, 1)
    stage([(z, 0, 1, 1, always), (z - 1, 0, 0, mine, first & (z > 0)), (z + 1, 0, 1, 1, first & (z < Z - 1))])

    @pl.when(helped)
    def _():
        give_part()

    @pl.when(z == 0)
    def _():
        finish(0)

    twin_wo(2)
    twin_wo(3)
    relay(1, 0, 0, second)
    relay(1, 0, 1, second)
    relay(2, 0, 1, first)
    relay(1, 1, 0, jnp.logical_not(helped))
    stage([(z - 1, 0, 0, mine, second & (z > 0)), (z + 2 - y, 0, 1, 1, z + 2 - y < Z), (z - 1, 1, 1, 1, (z > 0) & jnp.logical_not(helped))])

    @pl.when(z == 1)
    def _():
        finish(0)

    relay_half(2, 0, 0, 0, always)

    @pl.when(helps)
    def _():
        help_copy(0).wait_recv()
        _loop(0, 8, lambda u, _: full(z - u // 4, (u // 2) % 2, 2, u % 2))

    relay_half(2, 0, 1, 0, always)
    relay(3, 0, 1, first)
    relay(2, 0, 1, second)
    stage([(z - 2, 0, 0, jnp.where(helps, 2, mine), z >= 2), (z + 3 - y, 0, 1, 1, z + 3 - y < Z)])

    @pl.when(helps)
    def _():
        finish(0)

    for zz in range(Z):
        wo_copy(3, _sp(1 - y, zz, c)).wait_recv()
        wo_copy(4, _sp(1 - y, zz, c)).start()

    def helper_done():
        @pl.when(helps)
        def _():
            finish_help()

    last_unit = (jnp.where(helps, z - 2, jnp.where(helped, z - 3, z + 3)), jnp.where(helps, 1, 0), jnp.where(helped, 0, 1),
                 jnp.where(helps, 2, mine), helps | helped | (second & (z == 0)))
    for j in PAIR:
        relay_half(2, 1, j, 0, helps)
        relay_half(3, 0, j, 0, always)
        relay_half(3, 0, j, 1, second)
        stage([last_unit], (j,), helper_done if j else None)

    @pl.when(helped)
    def _():
        finish(0)

    @pl.when(jnp.logical_not(helped))
    def _():
        finish(1)

    for zz in range(Z):
        for yy in PAIR:
            wo_copy(4, _sp(yy, zz, 1 - c)).wait_recv()

    def result_wait(head):
        _send(og_s.at[head], og_s.at[head], o_send.at[head], o_recv.at[head], twin).wait_recv()

    @pl.when(served)
    def _():
        result_wait(h)

    @pl.when(jnp.logical_not(served))
    def _():
        og_s[h] = o_s[h]

    result_wait(beside_slot)
    low_rows = t // 2

    def output(n, two, final):
        at = pl.ds(pl.multiple_of(n * low_rows, 128), low_rows)
        if final:
            total = jnp.concatenate([mix_s[n, :low_rows, :low_rows], mix_s[n, :low_rows, low_rows:]], axis=0)
        else:
            total = x_ref[:, at].astype(jnp.float32)
        for head in two:
            there = pl.ds(pl.multiple_of(head * WIDE, WIDE), WIDE)
            total = total + jnp.dot(og_s[head], wo_s[there, at], preferred_element_type=jnp.float32)
        if final:
            y_ref[:, at] = total.astype(jnp.bfloat16)
        else:
            mix_s[n, :low_rows, :low_rows] = total[:low_rows]
            mix_s[n, :low_rows, low_rows:] = total[low_rows:]

    tiles = x_ref.shape[1] // low_rows
    _loop(0, tiles, lambda n, _: output(n, (h, beside_slot), False))
    result_wait(over)
    result_wait(diagonal_slot)
    _loop(0, tiles, lambda n, _: output(n, (over, diagonal_slot), True))

    for j in (1, 2, 3):
        @pl.when((c == x) | ((h + j) % 4 // 2 == y))
        def _():
            for i in range(3):
                w_give(i, j).wait_send()

        @pl.when(((h + j) % 4 < 2) | jnp.logical_not(helped))
        def _():
            result((h + j) % 4).wait_send()

    for which in PAIR:
        w_copy(2, _sp(1 - y, z, x), which).wait_send()
    for p in range(PIECES):
        a_copy(0, h, p).wait_send()
        a_copy(1, h, p).wait_send()
        a_copy(2, over, p).wait_send()
    for s in range(Z):
        for way in PAIR:
            source, there, on = arriving(s, way)

            @pl.when(there & on)
            def _():
                for yy in PAIR:
                    for which in PAIR:
                        w_copy(way, _sp(yy, source, x), which).wait_send()

                @pl.when(c == x)
                def _():
                    wo_copy(way, _sp(y, source, c)).wait_send()

            if s:

                @pl.when(there)
                def _():
                    for yy in PAIR:
                        for which in PAIR:
                            w_copy(2, _sp(yy, source, x), which).wait_send()

                    @pl.when(c == x)
                    def _():
                        wo_copy(2, _sp(y, source, c)).wait_send()

    for zz in range(Z):
        wo_copy(3, _sp(y, zz, c)).wait_send()
        wo_copy(4, _sp(y, zz, c)).wait_send()
        wo_copy(4, _sp(1 - y, zz, c)).wait_send()
    @pl.when(helped)
    def _():
        for i in range(3):
            help_copy(i).wait_send()

    @pl.when(helps)
    def _():
        for cc in PAIR:
            helped_result(cc).wait_send()

    for source in range(Z):
        for e in PAIR:
            for way in PAIR[: 2 - e]:

                @pl.when((z < Z - 1 - e) & (source <= z) if way == 0 else (z > 0) & (source >= z))
                def _():
                    for j in PAIR:
                        for copy in unit_copies(source, e, j, way):
                            copy.wait_send()


def solution(mesh):
    half = HEAD // 2
    freq = np.power(np.float32(THETA), -np.arange(half, dtype=np.float32) / np.float32(half)).astype(np.float32)[None]

    def step(x, gain, wq, wk, wv, wo):
        t, d = x.shape
        vmem, far = pl.BlockSpec(memory_space=pltpu.VMEM), pl.BlockSpec(memory_space=pl.ANY)
        low, dma = jnp.bfloat16, pltpu.SemaphoreType.DMA
        return pl.pallas_call(
            _kernel,
            out_shape=jax.ShapeDtypeStruct((t, d), low),
            in_specs=[vmem, vmem, far, far, far, far, vmem],
            out_specs=vmem,
            scratch_shapes=[
                pltpu.VMEM((4, t, d), low),
                pltpu.VMEM((d, 4 * HEAD), low),
                pltpu.VMEM((8 * HEAD, d), low),
                pltpu.VMEM((4 * t, half), jnp.float32),
                pltpu.VMEM((4 * t, half), jnp.float32),
                pltpu.VMEM((12, t, HEAD), low),
                pltpu.VMEM((Z, 2, 2, t, HEAD), low),
                pltpu.VMEM((Z, 2, 2, HEAD, t), low),
                pltpu.VMEM((12, 1, t), jnp.float32),
                pltpu.VMEM((12, HEAD + 8, t), jnp.float32),
                pltpu.VMEM((4, t, WIDE), low),
                pltpu.VMEM((4, t, WIDE), low),
                pltpu.VMEM((4, HEAD, t), low),
                pltpu.VMEM((4, 8, t), jnp.float32),
                pltpu.VMEM((2, t, WIDE), low),
                dma((4,)),
                dma((3, 4)),
                dma((3, 2, 16)),
                dma((3, 16)),
                dma((5, 16)),
                dma((16,)),
                dma((3, PIECES)),
                dma((4, PIECES)),
                dma((2, Z, 2, 2)),
                dma((Z, 2, 2)),
                dma((2, Z, 2, 2)),
                dma((Z, 2, 2)),
                dma((4,)),
                dma((4,)),
                dma((5,)),
                dma((3,)),
            ],
            compiler_params=pltpu.CompilerParams(collective_id=0, has_side_effects=True, vmem_limit_bytes=VMEM),
            cost_estimate=pl.CostEstimate(flops=2 * t * d * 6144 + 8 * t * 16 * t * 4 * HEAD, bytes_accessed=48 * 2**20, transcendentals=0),
        )(x, gain[None], wq, wk, wv, wo, jnp.asarray(freq))

    tokens, whole = P(("dp", "sp"), None), P("sp", None)
    return jax.shard_map(
        step,
        mesh=mesh,
        in_specs=(tokens, P(None), whole, whole, whole, whole),
        out_specs=tokens,
        check_vma=False,
    )
```

```python
import jax
import jax.numpy as jnp
import numpy as np
from jax import lax
from jax.experimental import pallas as pl
from jax.experimental.pallas import tpu as pltpu
from jax.sharding import PartitionSpec as P


NEG = -1e30
HIDDEN = 2 * NEG
LOG2E = 1.4426950408889634
VMEM = 67043328
HEAD = 256
THETA = 10000
Z = 4
PIECES = 4
WIDE = 512
PAIR = (0, 1)
MESH = pl.DeviceIdType.MESH


def _dot(a, b, ca, cb):
    return lax.dot_general(a, b, (((ca,), (cb,)), ((), ())), preferred_element_type=jnp.float32)


def _loop(first, last, body):
    lax.fori_loop(first, last, body, None)


def _sp(y, z, c):
    return (y * Z + z) * 2 + c


def _send(src, dst, send_sem, recv_sem, device):
    return pltpu.make_async_remote_copy(src_ref=src, dst_ref=dst, send_sem=send_sem, recv_sem=recv_sem, device_id=device, device_id_type=MESH)


def _meet(always, sometimes):
    barrier = pltpu.get_barrier_semaphore()
    count = len(always)
    for device in always:
        pl.semaphore_signal(barrier, inc=1, device_id=device, device_id_type=MESH)
    for there, device in sometimes:

        @pl.when(there)
        def _():
            pl.semaphore_signal(barrier, inc=1, device_id=device, device_id_type=MESH)

        count = count + there.astype(jnp.int32)
    pl.semaphore_wait(barrier, count)


def _kernel(x_ref, gain_ref, wq_ref, wk_ref, wv_ref, wo_ref, freq_ref, y_ref, a_s, w_s, wo_s, cos_s, sin_s, q_s, k_s, v_s, top_s, mix_s, o_s, og_s, part_s, stat_s, help_s,
            own_sem, w_first, w_send, w_recv, wo_send, wo_recv, a_send, a_recv, k_send, k_recv, v_send, v_recv, o_send, o_recv, help_send, help_recv):
    x = lax.axis_index("dp")
    me = lax.axis_index("sp")
    y, z, c = me // (2 * Z), (me // 2) % Z, me % 2
    h = 2 * y + c
    t, r, ro = x_ref.shape[0], wq_ref.shape[0], wo_ref.shape[0]
    part = t // PIECES
    e_scale = HEAD**-0.5 * LOG2E
    beside, across, corner, twin = (x, _sp(y, z, 1 - c)), (x, _sp(1 - y, z, c)), (x, _sp(1 - y, z, 1 - c)), (1 - x, me)
    along = [(x, _sp(y, jnp.minimum(z + 1, Z - 1), c)), (x, _sp(y, jnp.maximum(z - 1, 0), c))]
    goes = [z < Z - 1, z > 0]
    helps, helped = z == Z - 2, z == Z - 1
    taker, served = [(x, _sp(1, Z - 1, cc)) for cc in PAIR], helped & (y == 1)
    _meet([beside, across, corner, twin], list(zip(goes, along)) + [(helps, device) for device in taker]
          + [(served, (x, _sp(yy, Z - 2, cc))) for yy in PAIR for cc in PAIR])

    def w_rows(d):
        return pl.ds(pl.multiple_of(d * r, 16), r)

    column = [0, WIDE, 3 * HEAD, 4 * HEAD]
    given = [wq_ref, wk_ref, wv_ref]

    def w_part(i, head):
        wide = column[i + 1] - column[i]
        return given[i].at[:, pl.ds(pl.multiple_of(head * wide, 128), wide)]

    def w_place(i, d):
        return w_s.at[w_rows(d), column[i] : column[i + 1]]

    def w_give(i, j):
        to = (h + j) % 4
        return _send(w_part(i, to), w_place(i, me), w_first.at[i, j], w_recv.at[i, me], (x, _sp(to // 2, z, to % 2)))

    def w_given(yy, cc, which):
        d = _sp(yy, z, cc)
        for i in (1, 2) if which else (0,):
            _send(w_place(i, d), w_place(i, d), w_first.at[i, 0], w_recv.at[i, d], twin).wait_recv()

    def w_copy(kind, d, which):
        place = w_s.at[w_rows(d), WIDE * which : WIDE * (which + 1)]
        return _send(place, place, w_send.at[kind, which, d], w_recv.at[which, d], twin if kind == 2 else along[kind])

    def own_w(i):
        return pltpu.make_async_copy(w_part(i, h), w_place(i, me), own_sem.at[i])

    def wo_copy(kind, d):
        place = wo_s.at[pl.ds(pl.multiple_of(d * ro, 16), ro), :]
        if kind < 3:
            place = wo_s.at[pl.ds(pl.multiple_of(d * ro + x * (ro // 2), 16), ro // 2), :]
        return _send(place, place, wo_send.at[kind, d], wo_recv.at[kind // 2 % 2, d], [along[0], along[1], twin, across, beside][kind])

    def wo_twin_wait(d):
        place = wo_s.at[pl.ds(pl.multiple_of(d * ro + (1 - x) * (ro // 2), 16), ro // 2), :]
        _send(place, place, wo_send.at[2, d], wo_recv.at[1, d], twin).wait_recv()

    def own_wo():
        return pltpu.make_async_copy(wo_ref, wo_s.at[pl.ds(pl.multiple_of(me * ro, 16), ro), :], own_sem.at[3])

    def piece(slot, p):
        return a_s.at[slot, pl.ds(p * part, part), :]

    def a_copy(kind, slot, p):
        return _send(piece(slot, p), piece(slot, p), a_send.at[kind, p], a_recv.at[slot, p], across if kind == 1 else beside)

    over, diagonal_slot, beside_slot = 2 * (1 - y) + c, 2 * (1 - y) + 1 - c, 2 * y + 1 - c

    def relay_a(p):
        a_copy(1, over, p).wait_recv()
        a_copy(2, over, p).start()

    for which in (1, 0):
        for j in (1, 2, 3):

            @pl.when((c == x) | ((h + j) % 4 // 2 == y))
            def _():
                for i in (1, 2) if which else (0,):
                    w_give(i, j).start()

    for i in (1, 2, 0):
        own_w(i).start()
    own_wo().start()
    for p in range(PIECES):
        at = pl.ds(p * part, part)
        wide = x_ref[at, :].astype(jnp.float32)
        scale = lax.rsqrt(jnp.mean(wide * wide, -1, keepdims=True) + 1e-6)
        a_s[h, at, :] = (wide * scale * gain_ref[...].astype(jnp.float32)).astype(jnp.bfloat16)
        a_copy(1, h, p).start()
        a_copy(0, h, p).start()
    for i in range(3):
        own_w(i).wait()

    def give_w(which):
        for yy in PAIR:

            @pl.when(jnp.logical_not((c == x) & (y == yy)))
            def _():
                w_given(yy, x, which)

            @pl.when(y != yy)
            def _():
                w_copy(2, _sp(yy, z, x), which).start()

            for way in PAIR:

                @pl.when(goes[way])
                def _():
                    w_copy(way, _sp(yy, z, x), which).start()

    def arriving(s, way):
        source = z - s if way == 0 else z + s
        return source, (source >= 0) & (source < Z), goes[way]

    def pass_w(s, which):
        for way in PAIR:
            source, there, on = arriving(s, way)

            @pl.when(there)
            def _():
                for yy in PAIR:
                    w_copy(way, _sp(yy, source, x), which).wait_recv()

                    @pl.when(on)
                    def _():
                        w_copy(way, _sp(yy, source, x), which).start()

                    w_copy(2, _sp(yy, source, x), which).start()

    def w_rest(which):
        for yy in PAIR:
            for s in range(1, Z):
                w_copy(2, _sp(yy, (z + s) % Z, 1 - x), which).wait_recv()
        w_copy(2, _sp(1 - y, z, 1 - x), which).wait_recv()

        @pl.when(c == x)
        def _():
            w_given(y, 1 - x, which)

    def spread_wo(d):
        wo_copy(3, d).start()
        wo_copy(4, d).start()

    def pass_wo(s):
        for way in PAIR:
            source, there, on = arriving(s, way)

            @pl.when(there)
            def _():
                wo_copy(way, _sp(y, source, c)).wait_recv()

                @pl.when(on)
                def _():
                    wo_copy(way, _sp(y, source, c)).start()

                wo_copy(2, _sp(y, source, c)).start()

    def twin_wo(s):
        for way in PAIR:
            source, there, _ = arriving(s, way)

            @pl.when(there)
            def _():
                wo_twin_wait(_sp(y, source, c))
                spread_wo(_sp(y, source, c))

    give_w(1)

    step = min(256, t)

    def turn(i, _):
        slot, at = i // (t // step), (i % (t // step)) * step
        token = ((slot // 2) * Z + z) * 2 * t + (slot % 2) * t + at + lax.broadcasted_iota(jnp.int32, (step, HEAD // 2), 0)
        angle = token.astype(jnp.float32) * freq_ref[...]
        cos_s[pl.ds(i * step, step), :] = jnp.cos(angle)
        sin_s[pl.ds(i * step, step), :] = jnp.sin(angle)

    _loop(0, 4 * t // step, turn)
    for s in range(1, Z):
        pass_w(s, 1)
    give_w(0)
    own_wo().wait()

    for way in PAIR:

        @pl.when(goes[way])
        def _():
            wo_copy(way, me).start()

    spread_wo(me)
    w_rest(1)

    half = HEAD // 2
    always = z >= 0

    def turned(got, i, here):
        u, w = got[:, i * HEAD : i * HEAD + half], got[:, i * HEAD + half : (i + 1) * HEAD]
        cos, sin = cos_s[here, :], sin_s[here, :]
        return jnp.concatenate([u * cos - w * sin, w * cos + u * sin], -1).astype(jnp.bfloat16)

    def product(slot, at, columns):
        got = jnp.dot(a_s[slot, pl.ds(at, step), :], w_s[:, columns], preferred_element_type=jnp.float32)
        return got.astype(jnp.bfloat16).astype(jnp.float32)

    def keys_values(slot, at):
        got = product(slot, at, slice(WIDE, 4 * HEAD))
        there = pl.ds(pl.multiple_of(at, 128), step)
        k_s[z, slot // 2, slot % 2, there, :] = turned(got, 0, pl.ds(slot * t + at, step))
        v_s[z, slot // 2, slot % 2, :, there] = got[:, HEAD:].T.astype(jnp.bfloat16)

    def queries(slot, at):
        got = product(slot, at, slice(0, WIDE))
        for n in PAIR:
            q_s[slot * 2 + n, pl.ds(at, step), :] = turned(got, n, pl.ds(slot * t + at, step))

    per = t // step

    def unit_copies(source, e, j, way):
        k_at, v_at = k_s.at[source, e, j], v_s.at[source, e, j]
        return (
            _send(k_at, k_at, k_send.at[way, source, e, j], k_recv.at[source, e, j], along[way]),
            _send(v_at, v_at, v_send.at[way, source, e, j], v_recv.at[source, e, j], along[way]),
        )

    def pass_unit(source, e, j, way, when):
        @pl.when(when & (z < Z - 1 - e if way == 0 else z > 0))
        def _():
            for copy in unit_copies(source, e, j, way):
                copy.start()

    def give_unit(e):
        for j in PAIR:
            pass_unit(z, e, j, 0, always)
            pass_unit(z, e, j, 1, e == 0)

    for p in range(PIECES):
        a_copy(0, beside_slot, p).wait_recv()
    _loop(0, 2 * per, lambda i, _: keys_values(2 * y + i // per, (i % per) * step))
    for s in range(1, Z):
        pass_w(s, 0)
    pass_wo(1)
    give_unit(y)
    w_rest(0)
    _loop(0, 2 * per, lambda i, _: queries(2 * y + i // per, (i % per) * step))
    pass_wo(2)

    def others(i, _):
        for p in range(PIECES // per):
            relay_a(i * (PIECES // per) + p)
        keys_values(over, i * step)
        for p in range(PIECES // per):
            a_copy(2, diagonal_slot, i * (PIECES // per) + p).wait_recv()
        keys_values(diagonal_slot, i * step)

    _loop(0, per, others)
    give_unit(1 - y)

    def relay_half(s, e, j, way, when):
        source = z - s if way == 0 else z + s

        @pl.when(when & (source >= 0) & (source < Z))
        def _():
            for copy in unit_copies(source, e, j, way):
                copy.wait_recv()
            pass_unit(source, e, j, way, always)

    def relay(s, e, way, when):
        for j in PAIR:
            relay_half(s, e, j, way, when)

    first, second = y == 0, y == 1
    relay(1, 0, 0, first)
    relay(1, 0, 1, first)
    twin_wo(1)
    _loop(0, 2 * per, lambda i, _: queries(2 * (1 - y) + i // per, (i % per) * step))

    def help_copy(i):
        if i == 0:
            return _send(q_s.at[4:8], q_s.at[8:12], help_send.at[0], help_recv.at[0], along[1])
        place = part_s if i == 1 else stat_s
        return _send(place, place, help_send.at[i], help_recv.at[i], along[1])

    @pl.when(helped)
    def _():
        help_copy(0).start()

    pass_wo(3)

    top_s[...] = jnp.full(top_s.shape, NEG, jnp.float32)
    mix_s[...] = jnp.zeros(mix_s.shape, jnp.float32)
    ones = jnp.ones((8, t), jnp.bfloat16)

    def block(source, e, j, strips, masked):
        keys = k_s[source, e, j]
        values = jnp.concatenate([v_s[source, e, j], ones], axis=0)
        scores = [_dot(keys, q_s[i], 1, 1) for i in strips]
        weights, keeps = [], []
        for i, s in zip(strips, scores):
            if masked:
                ok = lax.broadcasted_iota(jnp.int32, (t, t), 1) >= lax.broadcasted_iota(jnp.int32, (t, t), 0)
                s = jnp.where(ok, s, HIDDEN)
            old = top_s[i]
            top = jnp.maximum(old, s.max(axis=0, keepdims=True))
            top_s[i] = top
            weights.append(jnp.exp2((s - top) * e_scale).astype(jnp.bfloat16))
            keeps.append(jnp.exp2((old - top) * e_scale))
        for i, p, keep in zip(strips, weights, keeps):
            mix_s[i] = mix_s[i] * keep + _dot(values, p, 1, 0)

    def full(source, e, g, j):
        block(source, e, j, [4 * g + i for i in range(4)], False)

    def diagonal(i, _):
        g, j = i // 2, i % 2
        block(z, g, j, [4 * g + 2 * j, 4 * g + 2 * j + 1], True)

    _loop(0, 4, diagonal)
    _loop(0, 2, lambda g, _: block(z, g, 0, [4 * g + 2, 4 * g + 3], False))

    def result(to):
        return _send(o_s.at[to], og_s.at[h], o_send.at[to], o_recv.at[h], (x, _sp(to // 2, z, to % 2)))

    def settle(i, s4, n):
        o_s[s4, :, n * HEAD : (n + 1) * HEAD] = (mix_s[i, :HEAD, :] * (1 / mix_s[i, HEAD : HEAD + 1, :])).astype(jnp.bfloat16).T

    def finish(g):
        def slot(i, _):
            s4 = 2 * g + i
            for n in PAIR:
                settle(2 * s4 + n, s4, n)

            @pl.when(s4 != h)
            def _():
                result(s4).start()

        _loop(0, 2, slot)

    def give_part():
        for n in range(4):
            i = 4 + n
            total = mix_s[i, HEAD : HEAD + 1, :]
            part_s[n] = (mix_s[i, :HEAD, :] * (1 / total)).astype(jnp.bfloat16)
            stat_s[n, 0:1, :] = top_s[i]
            stat_s[n, 1:2, :] = total
        help_copy(1).start()
        help_copy(2).start()

    def helped_result(cc):
        return _send(help_s.at[cc], og_s.at[h], help_send.at[3 + cc], o_recv.at[h], taker[cc])

    def finish_help():
        help_copy(1).wait_recv()
        help_copy(2).wait_recv()
        for cc in PAIR:
            for n in PAIR:
                i, k = 8 + 2 * cc + n, 2 * cc + n
                old, new = top_s[i], stat_s[k, 0:1, :]
                top = jnp.maximum(old, new)
                keep, gain = jnp.exp2((old - top) * e_scale), jnp.exp2((new - top) * e_scale) * stat_s[k, 1:2, :]
                total = mix_s[i, HEAD : HEAD + 1, :] * keep + gain
                both = mix_s[i, :HEAD, :] * keep + part_s[k].astype(jnp.float32) * gain
                help_s[cc, :, n * HEAD : (n + 1) * HEAD] = (both * (1 / total)).astype(jnp.bfloat16).T
            helped_result(cc).start()

    def stage(entries, halves=PAIR, then=None):
        per_strip = len(halves)

        def entry(k, _):
            def pick(n):
                got = jnp.asarray(entries[0][n])
                for i in range(1, len(entries)):
                    got = jnp.where(k == i, entries[i][n], got)
                return got

            source, e, least, most, go = (pick(n) for n in range(5))

            def work(u, _):
                full(source, e, most - u // per_strip, halves[0] + u % per_strip)
                if then is not None:

                    @pl.when(u == 0)
                    def _():
                        then()

            _loop(0, jnp.where(go, per_strip * (most + 1 - least), 0), work)

        _loop(0, len(entries), entry)

    mine = jnp.where(helped, 0, 1)
    stage([(z, 0, 1, 1, always), (z - 1, 0, 0, mine, first & (z > 0)), (z + 1, 0, 1, 1, first & (z < Z - 1))])

    @pl.when(helped)
    def _():
        give_part()

    @pl.when(z == 0)
    def _():
        finish(0)

    twin_wo(2)
    twin_wo(3)
    relay(1, 0, 0, second)
    relay(1, 0, 1, second)
    relay(2, 0, 1, first)
    relay(1, 1, 0, jnp.logical_not(helped))
    stage([(z - 1, 0, 0, mine, second & (z > 0)), (z + 2 - y, 0, 1, 1, z + 2 - y < Z), (z - 1, 1, 1, 1, (z > 0) & jnp.logical_not(helped))])

    @pl.when(z == 1)
    def _():
        finish(0)

    relay_half(2, 0, 0, 0, always)

    @pl.when(helps)
    def _():
        help_copy(0).wait_recv()
        _loop(0, 8, lambda u, _: full(z - u // 4, (u // 2) % 2, 2, u % 2))

    relay_half(2, 0, 1, 0, always)
    relay(3, 0, 1, first)
    relay(2, 0, 1, second)
    stage([(z - 2, 0, 0, jnp.where(helps, 2, mine), z >= 2), (z + 3 - y, 0, 1, 1, z + 3 - y < Z)])

    @pl.when(helps)
    def _():
        finish(0)

    for zz in range(Z):
        wo_copy(3, _sp(1 - y, zz, c)).wait_recv()
        wo_copy(4, _sp(1 - y, zz, c)).start()

    def helper_done():
        @pl.when(helps)
        def _():
            finish_help()

    last_unit = (jnp.where(helps, z - 2, jnp.where(helped, z - 3, z + 3)), jnp.where(helps, 1, 0), jnp.where(helped, 0, 1),
                 jnp.where(helps, 2, mine), helps | helped | (second & (z == 0)))
    for j in PAIR:
        relay_half(2, 1, j, 0, helps)
        relay_half(3, 0, j, 0, always)
        relay_half(3, 0, j, 1, second)
        stage([last_unit], (j,), helper_done if j else None)

    @pl.when(helped)
    def _():
        finish(0)

    @pl.when(jnp.logical_not(helped))
    def _():
        finish(1)

    for zz in range(Z):
        for yy in PAIR:
            wo_copy(4, _sp(yy, zz, 1 - c)).wait_recv()

    def result_wait(head):
        _send(og_s.at[head], og_s.at[head], o_send.at[head], o_recv.at[head], twin).wait_recv()

    early = (jnp.where(served, over, h), jnp.where(served, diagonal_slot, beside_slot))
    late = (jnp.where(served, h, over), jnp.where(served, beside_slot, diagonal_slot))

    @pl.when(served)
    def _():
        result_wait(over)

    @pl.when(jnp.logical_not(served))
    def _():
        og_s[h] = o_s[h]

    result_wait(early[1])
    low_rows = t // 2

    def output(n, two, final):
        at = pl.ds(pl.multiple_of(n * low_rows, 128), low_rows)
        if final:
            total = jnp.concatenate([mix_s[n, :low_rows, :low_rows], mix_s[n, :low_rows, low_rows:]], axis=0)
        else:
            total = x_ref[:, at].astype(jnp.float32)
        for head in two:
            there = pl.ds(pl.multiple_of(head * WIDE, WIDE), WIDE)
            total = total + jnp.dot(og_s[head], wo_s[there, at], preferred_element_type=jnp.float32)
        if final:
            y_ref[:, at] = total.astype(jnp.bfloat16)
        else:
            mix_s[n, :low_rows, :low_rows] = total[:low_rows]
            mix_s[n, :low_rows, low_rows:] = total[low_rows:]

    tiles = x_ref.shape[1] // low_rows
    _loop(0, tiles, lambda n, _: output(n, early, False))
    for head in late:
        result_wait(head)
    _loop(0, tiles, lambda n, _: output(n, late, True))

    for j in (1, 2, 3):
        @pl.when((c == x) | ((h + j) % 4 // 2 == y))
        def _():
            for i in range(3):
                w_give(i, j).wait_send()

        @pl.when(((h + j) % 4 < 2) | jnp.logical_not(helped))
        def _():
            result((h + j) % 4).wait_send()

    for which in PAIR:
        w_copy(2, _sp(1 - y, z, x), which).wait_send()
    for p in range(PIECES):
        a_copy(0, h, p).wait_send()
        a_copy(1, h, p).wait_send()
        a_copy(2, over, p).wait_send()
    for s in range(Z):
        for way in PAIR:
            source, there, on = arriving(s, way)

            @pl.when(there & on)
            def _():
                for yy in PAIR:
                    for which in PAIR:
                        w_copy(way, _sp(yy, source, x), which).wait_send()

                wo_copy(way, _sp(y, source, c)).wait_send()

            if s:

                @pl.when(there)
                def _():
                    for yy in PAIR:
                        for which in PAIR:
                            w_copy(2, _sp(yy, source, x), which).wait_send()

                    wo_copy(2, _sp(y, source, c)).wait_send()

    for zz in range(Z):
        wo_copy(3, _sp(y, zz, c)).wait_send()
        wo_copy(4, _sp(y, zz, c)).wait_send()
        wo_copy(4, _sp(1 - y, zz, c)).wait_send()
    @pl.when(helped)
    def _():
        for i in range(3):
            help_copy(i).wait_send()

    @pl.when(helps)
    def _():
        for cc in PAIR:
            helped_result(cc).wait_send()

    for source in range(Z):
        for e in PAIR:
            for way in PAIR[: 2 - e]:

                @pl.when((z < Z - 1 - e) & (source <= z) if way == 0 else (z > 0) & (source >= z))
                def _():
                    for j in PAIR:
                        for copy in unit_copies(source, e, j, way):
                            copy.wait_send()


def solution(mesh):
    half = HEAD // 2
    freq = np.power(np.float32(THETA), -np.arange(half, dtype=np.float32) / np.float32(half)).astype(np.float32)[None]

    def step(x, gain, wq, wk, wv, wo):
        t, d = x.shape
        vmem, far = pl.BlockSpec(memory_space=pltpu.VMEM), pl.BlockSpec(memory_space=pl.ANY)
        low, dma = jnp.bfloat16, pltpu.SemaphoreType.DMA
        return pl.pallas_call(
            _kernel,
            out_shape=jax.ShapeDtypeStruct((t, d), low),
            in_specs=[vmem, vmem, far, far, far, far, vmem],
            out_specs=vmem,
            scratch_shapes=[
                pltpu.VMEM((4, t, d), low),
                pltpu.VMEM((d, 4 * HEAD), low),
                pltpu.VMEM((8 * HEAD, d), low),
                pltpu.VMEM((4 * t, half), jnp.float32),
                pltpu.VMEM((4 * t, half), jnp.float32),
                pltpu.VMEM((12, t, HEAD), low),
                pltpu.VMEM((Z, 2, 2, t, HEAD), low),
                pltpu.VMEM((Z, 2, 2, HEAD, t), low),
                pltpu.VMEM((12, 1, t), jnp.float32),
                pltpu.VMEM((12, HEAD + 8, t), jnp.float32),
                pltpu.VMEM((4, t, WIDE), low),
                pltpu.VMEM((4, t, WIDE), low),
                pltpu.VMEM((4, HEAD, t), low),
                pltpu.VMEM((4, 8, t), jnp.float32),
                pltpu.VMEM((2, t, WIDE), low),
                dma((4,)),
                dma((3, 4)),
                dma((3, 2, 16)),
                dma((3, 16)),
                dma((5, 16)),
                dma((2, 16)),
                dma((3, PIECES)),
                dma((4, PIECES)),
                dma((2, Z, 2, 2)),
                dma((Z, 2, 2)),
                dma((2, Z, 2, 2)),
                dma((Z, 2, 2)),
                dma((4,)),
                dma((4,)),
                dma((5,)),
                dma((3,)),
            ],
            compiler_params=pltpu.CompilerParams(collective_id=0, has_side_effects=True, vmem_limit_bytes=VMEM),
            cost_estimate=pl.CostEstimate(flops=2 * t * d * 6144 + 8 * t * 16 * t * 4 * HEAD, bytes_accessed=48 * 2**20, transcendentals=0),
        )(x, gain[None], wq, wk, wv, wo, jnp.asarray(freq))

    tokens, whole = P(("dp", "sp"), None), P("sp", None)
    return jax.shard_map(
        step,
        mesh=mesh,
        in_specs=(tokens, P(None), whole, whole, whole, whole),
        out_specs=tokens,
        check_vma=False,
    )
```
